128 devices in a mesh: row: 16 (over x, z), col: 8 (over y, core).
Axes of the slice: x: 4, y: 4, z: 4, core: 2. Of those that a mesh axis runs over, the one named last changes fastest.
Arguments:
- panel_block: float32 [20480, 512], P('row', 'col'), may hold values from -12 to 12
- trailing: float32 [20480, 20480], P('row', 'col'), may hold values from -6 to 6
Outputs:
- updated: float32 [20480, 20480], P('row', 'col')
The draws below stay inside these ranges and needn't reach their ends.
All inputs are finite; a program needn't handle non-finite values.
Results may differ from the reference program's by a relative error of at most 0.0003.
Values sent between devices are 32-bit elements; how exact they have to be, the bound alone decides.
A program may use at most 128 MiB of HBM per device.

```python
import math
import jax
import jax.numpy as jnp
from jax import lax

N = 20480
K = 512
N_ROW = 16
N_COL = 8


def draw_panel_block(key, part):
    subkeys = jax.random.split(jax.random.fold_in(key, 11), 3)
    position = jnp.arange(N, dtype=jnp.float32) / N
    rising = 3.0 ** (position - 0.5)
    entries = jax.random.normal(subkeys[0], (N, K), jnp.float32)
    spread = 0.5
    row_scale = 10.0 ** jax.random.uniform(subkeys[1], (N, 1), jnp.float32, -spread, spread)
    col_scale = 10.0 ** jax.random.uniform(subkeys[2], (1, K), jnp.float32, -spread, spread)
    return entries * rising[:, None] * row_scale * col_scale / math.sqrt(K)


def steps_of(stream_key, dims, shards, low, top_value):
    gain, own = 1.0, jax.random.fold_in(stream_key, 6)
    for dim, blocks in shards:
        draws = jnp.exp(jax.random.uniform(jax.random.fold_in(own, dim), (blocks,), jnp.float32, low / len(shards), top_value / len(shards)))
        gain = gain * jnp.repeat(draws, dims[dim] // blocks).reshape([-1 if axis == dim else 1 for axis in range(len(dims))])
    return gain


def centred(own_key, shape, deviation, most, cuts=(), kind=jnp.bfloat16):
    values = deviation * jax.random.normal(own_key, shape, jnp.float32)
    if cuts:
        values = values * steps_of(own_key, shape, cuts, -0.22, 0.18)
    return jnp.clip(values, -most, most).astype(kind)


def setup_inputs(seed: int = 0) -> dict:
    seeds = jax.random.split(jax.random.key(seed), 3)
    panel_block = draw_panel_block(jax.random.fold_in(seeds[2], 71), 0)
    trailing = centred(seeds[1], (N, N), 1.0, 6.0, ((0, 16), (1, 8)), jnp.float32)
    return {"panel_block": panel_block, "trailing": trailing}


def reference(panel_block, trailing):
    local_rows = N // N_ROW
    local_cols = N // N_COL
    squares = jnp.sum(panel_block * panel_block)
    factor = 0.8 * jnp.sqrt(jnp.float32(N)) / jnp.sqrt(squares + 1e-06)
    matrix = panel_block.reshape(N_ROW, local_rows, K).transpose(1, 0, 2).reshape(N, K)
    column_rows = matrix.reshape(local_cols, N_COL, K).transpose(1, 0, 2).reshape(N, K)
    position = jnp.arange(N, dtype=jnp.int32)
    col_index = position % local_cols * N_COL + position // local_cols

    def one_block(pieces):
        row_block, slab_rows, source = pieces
        update = lax.dot_general(row_block, column_rows, (((1,), (1,)), ((), ())), precision=lax.Precision.HIGHEST, preferred_element_type=jnp.float32)
        row_index = jnp.arange(local_rows, dtype=jnp.int32) * N_ROW + source
        lower_part = row_index[:, None] >= col_index[None, :]
        return slab_rows - factor * jnp.where(lower_part, update, jnp.zeros_like(update))
    blocks = lax.map(one_block, (panel_block.reshape(N_ROW, local_rows, K), trailing.reshape(N_ROW, local_rows, N), jnp.arange(N_ROW, dtype=jnp.int32)))
    return blocks.reshape(N, N)
```

```python
import functools

import jax
import jax.numpy as jnp
from jax import lax
from jax.experimental import pallas as pl
from jax.experimental.pallas import tpu as pltpu
from jax.sharding import PartitionSpec as P

N = 20480
MESH = pl.DeviceIdType.MESH
LAG = 2
CHUNKS = 16
DEEPEST = 5
STEPS = CHUNKS + LAG * DEEPEST
TREE = {
    (0, 0): (0, (0,)),
    (1, 0): (1, (0, 1, 3)),
    (1, 3): (2, (0, 2, 3)),
    (1, 1): (2, (2,)),
    (2, 0): (2, (0, 1)),
    (2, 3): (3, (0,)),
    (1, 2): (3, (2,)),
    (0, 1): (3, ()),
    (0, 3): (3, ()),
    (2, 1): (3, (0, 1)),
    (3, 0): (3, ()),
    (2, 2): (4, (0,)),
    (0, 2): (4, ()),
    (3, 1): (4, ()),
    (3, 3): (4, ()),
    (3, 2): (5, ()),
}


def look_up(index, table):
    found = jnp.int32(0)
    for key, value in enumerate(table):
        found = jnp.where(index == key, jnp.int32(value), found)
    return found


def gather_kernel(
    block_ref, trailing_ref,
    t_ref, ah_ref, al_ref, bh_ref, bl_ref, sum_ref,
    at, b32, weave, sq_mine, sq_got,
    load_sem, trailing_sem, copy_sem, y_send, y_recv, d_send, d_recv,
    tree_send, tree_recv, sq_send, sq_recv,
):
    row = lax.axis_index("row")
    col = lax.axis_index("col")
    x, z = row // 4, row % 4
    y, core = col // 2, col % 2

    def device(dx=0, dy=0, dz=0):
        return ((x + dx) % 4 * 4 + (z + dz) % 4, (y + dy) % 4 * 2 + core)

    partner = (row, y * 2 + 1 - core)
    y_up, y_down = device(dy=1), device(dy=3)
    around = (device(dx=1), device(dz=1), device(dx=3), device(dz=3))

    trailing_copy = pltpu.make_async_copy(trailing_ref, t_ref, trailing_sem)
    own = pl.multiple_of(col * 64, 64)
    load = pltpu.make_async_copy(block_ref, at.at[pl.ds(own, 64)], load_sem)
    load.start()
    barrier = pltpu.get_barrier_semaphore()
    for peer in (partner, y_up, y_down, *around):
        pl.semaphore_signal(barrier, inc=1, device_id=peer, device_id_type=MESH)
    load.wait()
    trailing_copy.start()
    value = at[pl.ds(own, 64), :]
    square = jnp.sum((value * value).reshape(8, 8, 1280), axis=0)
    total = square[:, 0:128]
    for tile in range(1, 10):
        total = total + square[:, 128 * tile : 128 * tile + 128]
    sq_mine[0] = total
    pl.semaphore_wait(barrier, 7)

    def half(y_off, same, h):
        owner = (y + y_off) % 4 * 2 + (core if same else 1 - core)
        return pl.ds(pl.multiple_of(owner * 64 + 32 * h, 32), 32)

    def send(rows, send_sem, recv_sem, to):
        return pltpu.make_async_remote_copy(
            src_ref=at.at[rows], dst_ref=at.at[rows], send_sem=send_sem, recv_sem=recv_sem,
            device_id=to, device_id_type=MESH,
        )

    for h in (0, 1):
        send(half(0, True, h), y_send.at[0], y_recv.at[2 + h], y_up).start()
        send(half(0, True, h), y_send.at[1], y_recv.at[h], y_down).start()
        send(half(0, True, h), d_send, d_recv.at[h], partner).start()

    def got_y(index, y_off, h):
        send(half(y_off, True, h), y_send.at[0], y_recv.at[index], y_up).wait_recv()

    def got_d(index, y_off, h):
        send(half(y_off, False, h), d_send, d_recv.at[index], partner).wait_recv()

    def over(index, y_off, h):
        send(half(y_off, True, h), d_send, d_recv.at[index], partner).start()

    def quarter(rel):
        return pl.ds(pl.multiple_of((y + rel) % 4 * 128, 128), 128)

    roots = []
    plans = []
    for p in range(2):
        u = (x - (y // 2 + 2 * p)) % 4
        v = (z - (y % 2 * 2 + core)) % 4
        roots.append((u == 0) & (v == 0))
        for t in range(4):
            cu, cv = ((u, v), (v, (4 - u) % 4), ((4 - u) % 4, (4 - v) % 4), ((4 - v) % 4, u))[t]
            table = [TREE[i // 4, i % 4] for i in range(16)]
            code = look_up(cu * 4 + cv, [d + 8 * sum(1 << k for k in kids) for d, kids in table])
            plans.append((p, t, code % 8, code // 8))

    def own_copy(p, rel):
        rows = quarter(rel)
        return pltpu.make_async_copy(at.at[rows], b32.at[p, rows], copy_sem.at[p, rel])

    def convert(rel):
        for p in range(2):
            @pl.when(roots[p])
            def _():
                own_copy(p, rel).wait()
        rows = quarter(rel)
        cols = slice(128 * rel, 128 * rel + 128)

        @pl.loop(0, 10)
        def _(n):
            lanes = pl.ds(pl.multiple_of(n * 128, 128), 128)
            a = at[rows, lanes].T
            high = a.astype(jnp.bfloat16)
            ah_ref[lanes, cols] = high
            al_ref[lanes, cols] = (a - high.astype(jnp.float32)).astype(jnp.bfloat16)
            wide = pl.ds(pl.multiple_of(n * 256, 256), 256)
            for p in range(2):
                weave[n % 2, pl.ds(p, 128, stride=2), :] = b32[p, rows, lanes].T
            b = weave[n % 2]
            high = b.astype(jnp.bfloat16)
            bh_ref[wide, cols] = high
            bl_ref[wide, cols] = (b - high.astype(jnp.float32)).astype(jnp.bfloat16)

    def sq_peer(e):
        flip_x = jnp.where(e == 3, x + 1 - 2 * (x % 2), jnp.where(e == 4, 3 - x, x))
        flip_z = jnp.where(e == 5, z + 1 - 2 * (z % 2), jnp.where(e == 6, 3 - z, z))
        flip_y = jnp.where(e == 1, y + 1 - 2 * (y % 2), jnp.where(e == 2, 3 - y, y))
        flip_core = jnp.where(e == 0, 1 - core, core)
        return (flip_x * 4 + flip_z, flip_y * 2 + flip_core)

    def sq_copy(e):
        return pltpu.make_async_remote_copy(
            src_ref=sq_mine.at[e], dst_ref=sq_got.at[e], send_sem=sq_send.at[e], recv_sem=sq_recv.at[e],
            device_id=sq_peer(e), device_id_type=MESH,
        )

    def chunk_rows(c, t):
        group, low = c // 4, c % 2
        middle = (group == 1) | (group == 2)
        h = jnp.where(middle, group - 1, low)
        y_off = jnp.where(middle, 1 + 2 * low, jnp.where(group == 0, 0, 2))
        owner = (y + y_off) % 4 * 2 + (core + c // 2) % 2
        return pl.ds(pl.multiple_of(owner * 64 + 32 * h + 8 * t, 8), 8)

    @pl.loop(0, STEPS)
    def _(s):
        @pl.when(s == 2)
        def _():
            got_d(0, 0, 0)
            got_d(1, 0, 1)

        @pl.when(s == 4)
        def _():
            got_y(2, 3, 0)
            send(half(3, True, 0), y_send.at[2], y_recv.at[4], y_up).start()
            over(4, 3, 0)
            got_y(0, 1, 0)
            over(2, 1, 0)
            for p in range(2):
                @pl.when(roots[p])
                def _():
                    own_copy(p, 0).start()

        @pl.when(s == 6)
        def _():
            got_d(2, 1, 0)
            got_d(4, 3, 0)

        @pl.when(s == 8)
        def _():
            got_y(1, 1, 1)
            send(half(1, True, 1), y_send.at[3], y_recv.at[5], y_down).start()
            over(3, 1, 1)
            got_y(3, 3, 1)
            over(5, 3, 1)

        @pl.when(s == 10)
        def _():
            got_d(3, 1, 1)
            got_d(5, 3, 1)
            for p in range(2):
                @pl.when(roots[p])
                def _():
                    own_copy(p, 1).start()
                    own_copy(p, 3).start()

        @pl.when(s == 12)
        def _():
            got_y(4, 2, 0)
            over(6, 2, 0)
            got_y(5, 2, 1)
            over(7, 2, 1)

        @pl.when(s == 14)
        def _():
            got_d(6, 2, 0)
            got_d(7, 2, 1)
            for p in range(2):
                @pl.when(roots[p])
                def _():
                    own_copy(p, 2).start()

        for p, t, depth, kids in plans:
            c = s - LAG * depth
            live = (c >= 0) & (c < CHUNKS)
            rows = chunk_rows(c, t)

            def forward(src, d, c=c, rows=rows, p=p, t=t):
                return pltpu.make_async_remote_copy(
                    src_ref=src, dst_ref=b32.at[p, rows],
                    send_sem=tree_send.at[p, t, d], recv_sem=tree_recv.at[p, t, c],
                    device_id=around[(d + t) % 4], device_id_type=MESH,
                )

            @pl.when(live & (depth == 0))
            def _():
                forward(at.at[rows], 0).start()

            @pl.when(live & (depth > 0))
            def _():
                forward(b32.at[p, rows], 0).wait_recv()
                for d in range(4):
                    @pl.when(kids // (1 << d) % 2 == 1)
                    def _():
                        forward(b32.at[p, rows], d).start()

        @pl.when((s % 2 == 0) & (s < 14))
        def _():
            sq_copy(s // 2).start()

        @pl.when((s % 2 == 1) & (s < 14))
        def _():
            e = s // 2
            sq_copy(e).wait_recv()
            sq_mine[e + 1] = sq_mine[e] + sq_got[e]

        @pl.when(s == 3 + LAG * DEEPEST)
        def _():
            convert(0)

        @pl.when(s == 11 + LAG * DEEPEST)
        def _():
            convert(1)

        @pl.when(s == 12 + LAG * DEEPEST)
        def _():
            convert(3)

    convert(2)
    sum_ref[...] = sq_mine[7]

    def sent(sem, rows):
        return pltpu.make_async_remote_copy(
            src_ref=at.at[pl.ds(0, rows)], dst_ref=at.at[pl.ds(0, rows)], send_sem=sem, recv_sem=sem,
            device_id=partner, device_id_type=MESH,
        ).wait_send()

    for p, t, depth, kids in plans:
        for d in range(4):
            @pl.when(kids // (1 << d) % 2 == 1)
            def _():
                sent(tree_send.at[p, t, d], CHUNKS * 8)

    sent(y_send.at[0], 64)
    sent(y_send.at[1], 64)
    sent(y_send.at[2], 32)
    sent(y_send.at[3], 32)
    sent(d_send, 256)

    @pl.loop(0, 7)
    def _(e):
        sq_copy(e).wait_send()

    trailing_copy.wait()


def update_kernel(t_ref, ah_ref, al_ref, bh_ref, bl_ref, sum_ref, out_ref, stage, upper_sem, tile_sem):
    row = lax.axis_index("row")
    col = lax.axis_index("col")
    dot = functools.partial(
        lax.dot_general, dimension_numbers=(((1,), (1,)), ((), ())), preferred_element_type=jnp.float32
    )

    def upper(a):
        where = (pl.ds(256 * a, 256), pl.ds(512 * (a + 1), 2560 - 512 * (a + 1)))
        return pltpu.make_async_copy(t_ref.at[where], out_ref.at[where], upper_sem.at[a])

    def tile_copy(a, b):
        where = (pl.ds(256 * a, 256), pl.ds(512 * b, 512))
        return pltpu.make_async_copy(stage.at[where], out_ref.at[where], tile_sem.at[a, b])

    for a in range(4):
        upper(a).start()
    squares = jnp.sum(sum_ref[...])
    factor = 0.8 * jnp.sqrt(jnp.float32(N)) / jnp.sqrt(jnp.full((256, 512), squares, jnp.float32) + 1e-6)

    @pl.loop(0, 5)
    def _(a):
        @pl.loop(0, a + 1)
        def _(b):
            rows = pl.ds(pl.multiple_of(a * 256, 256), 256)
            cols = pl.ds(pl.multiple_of(b * 512, 512), 512)
            ah, bh = ah_ref[rows, :], bh_ref[cols, :]
            update = dot(ah, bh) + dot(ah, bl_ref[cols, :]) + dot(al_ref[rows, :], bh)
            i = lax.broadcasted_iota(jnp.int32, (256, 512), 0)
            j = lax.broadcasted_iota(jnp.int32, (256, 512), 1)
            lower = (a * 256 + i) * 16 + row >= (b * 512 + j) * 8 + col
            stage[rows, cols] = t_ref[rows, cols] - factor * jnp.where(lower, update, 0.0)
            copy = pltpu.make_async_copy(stage.at[rows, cols], out_ref.at[rows, cols], tile_sem.at[a, b])
            copy.start()

    for a in range(4):
        upper(a).wait()
    for a in range(5):
        for b in range(a + 1):
            tile_copy(a, b).wait()


def on_device(panel_block, trailing):
    bf16 = jnp.bfloat16
    f32 = jnp.float32
    dma = pltpu.SemaphoreType.DMA
    anywhere = pl.BlockSpec(memory_space=pl.ANY)
    vmem = pl.BlockSpec(memory_space=pltpu.VMEM)
    gathered = pl.pallas_call(
        gather_kernel,
        out_shape=(
            pltpu.VMEM((1280, 2560), f32),
            pltpu.VMEM((1280, 512), bf16),
            pltpu.VMEM((1280, 512), bf16),
            pltpu.VMEM((2560, 512), bf16),
            pltpu.VMEM((2560, 512), bf16),
            pltpu.VMEM((8, 128), f32),
        ),
        in_specs=[anywhere, anywhere],
        out_specs=[vmem] * 6,
        scratch_shapes=[
            pltpu.VMEM((512, 1280), f32),
            pltpu.VMEM((2, 512, 1280), f32),
            pltpu.VMEM((2, 256, 128), f32),
            pltpu.VMEM((8, 8, 128), f32),
            pltpu.VMEM((7, 8, 128), f32),
            dma(()), dma(()), dma((2, 4)), dma((4,)), dma((6,)), dma(()), dma((8,)),
            dma((2, 4, 4)), dma((2, 4, CHUNKS)), dma((7,)), dma((7,)),
        ],
        compiler_params=pltpu.CompilerParams(
            collective_id=0, has_side_effects=True, vmem_limit_bytes=12 * 1024 * 1024
        ),
        name="gather",
    )(panel_block.T, trailing)
    return pl.pallas_call(
        update_kernel,
        out_shape=jax.ShapeDtypeStruct((1280, 2560), f32),
        in_specs=[vmem] * 6,
        out_specs=anywhere,
        scratch_shapes=[pltpu.VMEM((1280, 2560), f32), dma((4,)), dma((5, 5))],
        compiler_params=pltpu.CompilerParams(vmem_limit_bytes=24 * 1024 * 1024),
        name="update",
    )(*gathered)


def solution(mesh):
    return jax.shard_map(
        on_device,
        mesh=mesh,
        in_specs=(P("row", "col"), P("row", "col")),
        out_specs=P("row", "col"),
        check_vma=False,
    )
```

```python
import functools

import jax
import jax.numpy as jnp
from jax import lax
from jax.experimental import pallas as pl
from jax.experimental.pallas import tpu as pltpu
from jax.sharding import PartitionSpec as P

N = 20480
MESH = pl.DeviceIdType.MESH
LAG = 2
CHUNKS = 16
DEEPEST = 5
STEPS = CHUNKS + LAG * DEEPEST
TREE = {
    (0, 0): (0, (0,)),
    (1, 0): (1, (0, 1, 3)),
    (1, 3): (2, (0, 2, 3)),
    (1, 1): (2, (2,)),
    (2, 0): (2, (0, 1)),
    (2, 3): (3, (0,)),
    (1, 2): (3, (2,)),
    (0, 1): (3, ()),
    (0, 3): (3, ()),
    (2, 1): (3, (0, 1)),
    (3, 0): (3, ()),
    (2, 2): (4, (0,)),
    (0, 2): (4, ()),
    (3, 1): (4, ()),
    (3, 3): (4, ()),
    (3, 2): (5, ()),
}


def look_up(index, table):
    found = jnp.int32(0)
    for key, value in enumerate(table):
        found = jnp.where(index == key, jnp.int32(value), found)
    return found


def gather_kernel(
    block_ref, trailing_ref,
    t_ref, acc_ref, a_last, b_last, sum_ref,
    at, b32, a_cat, b_cat, weave, sq_mine, sq_got,
    load_sem, trailing_sem, copy_sem, y_send, y_recv, d_send, d_recv,
    tree_send, tree_recv, sq_send, sq_recv,
):
    row = lax.axis_index("row")
    col = lax.axis_index("col")
    x, z = row // 4, row % 4
    y, core = col // 2, col % 2

    def device(dx=0, dy=0, dz=0):
        return ((x + dx) % 4 * 4 + (z + dz) % 4, (y + dy) % 4 * 2 + core)

    partner = (row, y * 2 + 1 - core)
    y_up, y_down = device(dy=1), device(dy=3)
    around = (device(dx=1), device(dz=1), device(dx=3), device(dz=3))

    trailing_copy = pltpu.make_async_copy(trailing_ref, t_ref, trailing_sem)
    own = pl.multiple_of(col * 64, 64)
    load = pltpu.make_async_copy(block_ref, at.at[pl.ds(own, 64)], load_sem)
    load.start()
    barrier = pltpu.get_barrier_semaphore()
    for peer in (partner, y_up, y_down, *around):
        pl.semaphore_signal(barrier, inc=1, device_id=peer, device_id_type=MESH)
    load.wait()
    trailing_copy.start()
    value = at[pl.ds(own, 64), :]
    square = jnp.sum((value * value).reshape(8, 8, 1280), axis=0)
    total = square[:, 0:128]
    for tile in range(1, 10):
        total = total + square[:, 128 * tile : 128 * tile + 128]
    sq_mine[0] = total
    pl.semaphore_wait(barrier, 7)

    def half(y_off, same, h):
        owner = (y + y_off) % 4 * 2 + (core if same else 1 - core)
        return pl.ds(pl.multiple_of(owner * 64 + 32 * h, 32), 32)

    def send(rows, send_sem, recv_sem, to):
        return pltpu.make_async_remote_copy(
            src_ref=at.at[rows], dst_ref=at.at[rows], send_sem=send_sem, recv_sem=recv_sem,
            device_id=to, device_id_type=MESH,
        )

    for h in (0, 1):
        send(half(0, True, h), y_send.at[0], y_recv.at[2 + h], y_up).start()
        send(half(0, True, h), y_send.at[1], y_recv.at[h], y_down).start()
        send(half(0, True, h), d_send, d_recv.at[h], partner).start()

    def got_y(index, y_off, h):
        send(half(y_off, True, h), y_send.at[0], y_recv.at[index], y_up).wait_recv()

    def got_d(index, y_off, h):
        send(half(y_off, False, h), d_send, d_recv.at[index], partner).wait_recv()

    def over(index, y_off, h):
        send(half(y_off, True, h), d_send, d_recv.at[index], partner).start()

    def quarter(rel):
        return pl.ds(pl.multiple_of((y + rel) % 4 * 128, 128), 128)

    roots = []
    plans = []
    for p in range(2):
        u = (x - (y // 2 + 2 * p)) % 4
        v = (z - (y % 2 * 2 + core)) % 4
        roots.append((u == 0) & (v == 0))
        for t in range(4):
            cu, cv = ((u, v), (v, (4 - u) % 4), ((4 - u) % 4, (4 - v) % 4), ((4 - v) % 4, u))[t]
            table = [TREE[i // 4, i % 4] for i in range(16)]
            code = look_up(cu * 4 + cv, [d + 8 * sum(1 << k for k in kids) for d, kids in table])
            plans.append((p, t, code % 8, code // 8))

    def own_copy(p, rel):
        rows = quarter(rel)
        return pltpu.make_async_copy(at.at[rows], b32.at[p, rows], copy_sem.at[p, rel])

    def convert(rel, first=0, last=10):
        if first == 0:
            for p in range(2):
                @pl.when(roots[p])
                def _():
                    own_copy(p, rel).wait()
        rows = quarter(rel)
        a_to, b_to, base = (a_last, b_last, 0) if rel == 2 else (a_cat, b_cat, 384 * (0, 1, None, 2)[rel])

        def split(value):
            high = value.astype(jnp.bfloat16)
            return high, (value - high.astype(jnp.float32)).astype(jnp.bfloat16)

        @pl.loop(first, last, unroll=2)
        def _(n):
            lanes = pl.ds(pl.multiple_of(n * 128, 128), 128)
            high, low = split(at[rows, lanes].T)
            for k, part in enumerate((high, high, low)):
                a_to[lanes, base + 128 * k : base + 128 * k + 128] = part
            for p in range(2):
                weave[n % 2, pl.ds(p, 128, stride=2), :] = b32[p, rows, lanes].T
            wide = pl.ds(pl.multiple_of(n * 256, 256), 256)
            high, low = split(weave[n % 2])
            for k, part in enumerate((high, low, high)):
                b_to[wide, base + 128 * k : base + 128 * k + 128] = part

    def product(b, start, stop):
        rows, cols = slice(256 * b, 1280), slice(512 * b, 512 * b + 512)
        return lax.dot_general(
            a_cat[rows, start:stop], b_cat[cols, start:stop],
            (((1,), (1,)), ((), ())), preferred_element_type=jnp.float32,
        )

    def sq_peer(e):
        flip_x = jnp.where(e == 3, x + 1 - 2 * (x % 2), jnp.where(e == 4, 3 - x, x))
        flip_z = jnp.where(e == 5, z + 1 - 2 * (z % 2), jnp.where(e == 6, 3 - z, z))
        flip_y = jnp.where(e == 1, y + 1 - 2 * (y % 2), jnp.where(e == 2, 3 - y, y))
        flip_core = jnp.where(e == 0, 1 - core, core)
        return (flip_x * 4 + flip_z, flip_y * 2 + flip_core)

    def sq_copy(e):
        return pltpu.make_async_remote_copy(
            src_ref=sq_mine.at[e], dst_ref=sq_got.at[e], send_sem=sq_send.at[e], recv_sem=sq_recv.at[e],
            device_id=sq_peer(e), device_id_type=MESH,
        )

    def chunk_rows(c, t):
        group, low = c // 4, c % 2
        middle = (group == 1) | (group == 2)
        h = jnp.where(middle, group - 1, low)
        y_off = jnp.where(middle, 1 + 2 * low, jnp.where(group == 0, 0, 2))
        owner = (y + y_off) % 4 * 2 + (core + c // 2) % 2
        return pl.ds(pl.multiple_of(owner * 64 + 32 * h + 8 * t, 8), 8)

    @pl.loop(0, STEPS)
    def _(s):
        @pl.when(s == 2)
        def _():
            got_d(0, 0, 0)
            got_d(1, 0, 1)

        @pl.when(s == 4)
        def _():
            got_y(2, 3, 0)
            send(half(3, True, 0), y_send.at[2], y_recv.at[4], y_up).start()
            over(4, 3, 0)
            got_y(0, 1, 0)
            over(2, 1, 0)
            for p in range(2):
                @pl.when(roots[p])
                def _():
                    own_copy(p, 0).start()

        @pl.when(s == 6)
        def _():
            got_d(2, 1, 0)
            got_d(4, 3, 0)

        @pl.when(s == 8)
        def _():
            got_y(1, 1, 1)
            send(half(1, True, 1), y_send.at[3], y_recv.at[5], y_down).start()
            over(3, 1, 1)
            got_y(3, 3, 1)
            over(5, 3, 1)

        @pl.when(s == 10)
        def _():
            got_d(3, 1, 1)
            got_d(5, 3, 1)
            for p in range(2):
                @pl.when(roots[p])
                def _():
                    own_copy(p, 1).start()
                    own_copy(p, 3).start()

        @pl.when(s == 12)
        def _():
            got_y(4, 2, 0)
            over(6, 2, 0)
            got_y(5, 2, 1)
            over(7, 2, 1)

        @pl.when(s == 14)
        def _():
            got_d(6, 2, 0)
            got_d(7, 2, 1)
            for p in range(2):
                @pl.when(roots[p])
                def _():
                    own_copy(p, 2).start()

        for p, t, depth, kids in plans:
            c = s - LAG * depth
            live = (c >= 0) & (c < CHUNKS)
            rows = chunk_rows(c, t)

            def forward(src, d, c=c, rows=rows, p=p, t=t):
                return pltpu.make_async_remote_copy(
                    src_ref=src, dst_ref=b32.at[p, rows],
                    send_sem=tree_send.at[p, t, d], recv_sem=tree_recv.at[p, t, c],
                    device_id=around[(d + t) % 4], device_id_type=MESH,
                )

            @pl.when(live & (depth == 0))
            def _():
                forward(at.at[rows], 0).start()

            @pl.when(live & (depth > 0))
            def _():
                forward(b32.at[p, rows], 0).wait_recv()
                for d in range(4):
                    @pl.when(kids // (1 << d) % 2 == 1)
                    def _():
                        forward(b32.at[p, rows], d).start()

        @pl.when((s % 2 == 0) & (s < 14))
        def _():
            sq_copy(s // 2).start()

        @pl.when((s % 2 == 1) & (s < 14))
        def _():
            e = s // 2
            sq_copy(e).wait_recv()
            sq_mine[e + 1] = sq_mine[e] + sq_got[e]

        ready = 3 + LAG * DEEPEST
        for k in range(5):
            @pl.when(s == ready + k)
            def _():
                convert(0, 2 * k, 2 * k + 2)

            @pl.when(s == ready + 5 + k)
            def _():
                acc_ref[256 * k : 1280, 512 * k : 512 * k + 512] = product(k, 0, 384)

    convert(1)
    convert(3)
    for k in range(5):
        acc_ref[256 * k : 1280, 512 * k : 512 * k + 512] += product(k, 384, 1152)
    convert(2)
    sum_ref[...] = sq_mine[7]

    def sent(sem, rows):
        return pltpu.make_async_remote_copy(
            src_ref=at.at[pl.ds(0, rows)], dst_ref=at.at[pl.ds(0, rows)], send_sem=sem, recv_sem=sem,
            device_id=partner, device_id_type=MESH,
        ).wait_send()

    for p, t, depth, kids in plans:
        for d in range(4):
            @pl.when(kids // (1 << d) % 2 == 1)
            def _():
                sent(tree_send.at[p, t, d], CHUNKS * 8)

    sent(y_send.at[0], 64)
    sent(y_send.at[1], 64)
    sent(y_send.at[2], 32)
    sent(y_send.at[3], 32)
    sent(d_send, 256)

    @pl.loop(0, 7)
    def _(e):
        sq_copy(e).wait_send()

    trailing_copy.wait()


def update_kernel(t_ref, acc_ref, a_ref, b_ref, sum_ref, out_ref, stage, upper_sem, lower_sem):
    row = lax.axis_index("row")
    col = lax.axis_index("col")

    def upper(a):
        where = (pl.ds(256 * a, 256), pl.ds(512 * (a + 1), 2560 - 512 * (a + 1)))
        return pltpu.make_async_copy(t_ref.at[where], out_ref.at[where], upper_sem.at[a])

    def lower(b):
        where = (pl.ds(256 * b, 1280 - 256 * b), pl.ds(512 * b, 512))
        return pltpu.make_async_copy(stage.at[where], out_ref.at[where], lower_sem.at[b])

    for a in range(4):
        upper(a).start()
    squares = jnp.full((8, 512), jnp.sum(sum_ref[...]), jnp.float32)
    factor = (0.8 * jnp.sqrt(jnp.float32(N)) / jnp.sqrt(squares + 1e-6))[0:1, :]
    i = lax.broadcasted_iota(jnp.int32, (256, 512), 0)
    j = lax.broadcasted_iota(jnp.int32, (256, 512), 1)
    for b in range(5):
        cols = slice(512 * b, 512 * b + 512)
        update = acc_ref[256 * b : 1280, cols] + lax.dot_general(
            a_ref[256 * b : 1280, :], b_ref[cols, :],
            (((1,), (1,)), ((), ())), preferred_element_type=jnp.float32,
        )
        edge = slice(256 * b, 256 * b + 256)
        below = (256 * b + i) * 16 + row >= (512 * b + j) * 8 + col
        stage[edge, cols] = t_ref[edge, cols] - factor * jnp.where(below, update[0:256], 0.0)
        if b < 4:
            rest = slice(256 * b + 256, 1280)
            stage[rest, cols] = t_ref[rest, cols] - factor * update[256:]
        lower(b).start()
    for a in range(4):
        upper(a).wait()
    for b in range(5):
        lower(b).wait()


def on_device(panel_block, trailing):
    bf16 = jnp.bfloat16
    f32 = jnp.float32
    dma = pltpu.SemaphoreType.DMA
    anywhere = pl.BlockSpec(memory_space=pl.ANY)
    in_hbm = functools.partial(pltpu.with_memory_space_constraint, memory_space=pltpu.HBM)
    vmem = pl.BlockSpec(memory_space=pltpu.VMEM)
    gathered = pl.pallas_call(
        gather_kernel,
        out_shape=(
            pltpu.VMEM((1280, 2560), f32),
            pltpu.VMEM((1280, 2560), f32),
            pltpu.VMEM((1280, 384), bf16),
            pltpu.VMEM((2560, 384), bf16),
            pltpu.VMEM((8, 128), f32),
        ),
        in_specs=[anywhere, anywhere],
        out_specs=[vmem] * 5,
        scratch_shapes=[
            pltpu.VMEM((512, 1280), f32),
            pltpu.VMEM((2, 512, 1280), f32),
            pltpu.VMEM((1280, 1152), bf16),
            pltpu.VMEM((2560, 1152), bf16),
            pltpu.VMEM((2, 256, 128), f32),
            pltpu.VMEM((8, 8, 128), f32),
            pltpu.VMEM((7, 8, 128), f32),
            dma(()), dma(()), dma((2, 4)), dma((4,)), dma((6,)), dma(()), dma((8,)),
            dma((2, 4, 4)), dma((2, 4, CHUNKS)), dma((7,)), dma((7,)),
        ],
        compiler_params=pltpu.CompilerParams(
            collective_id=0, has_side_effects=True, vmem_limit_bytes=24 * 1024 * 1024
        ),
        name="gather",
    )(in_hbm(panel_block.T), in_hbm(trailing))
    return pl.pallas_call(
        update_kernel,
        out_shape=jax.ShapeDtypeStruct((1280, 2560), f32),
        in_specs=[vmem] * 5,
        out_specs=anywhere,
        scratch_shapes=[pltpu.VMEM((1280, 2560), f32), dma((4,)), dma((5,))],
        compiler_params=pltpu.CompilerParams(vmem_limit_bytes=24 * 1024 * 1024),
        name="update",
    )(*gathered)


def solution(mesh):
    return jax.shard_map(
        on_device,
        mesh=mesh,
        in_specs=(P("row", "col"), P("row", "col")),
        out_specs=P("row", "col"),
        check_vma=False,
    )
```

```python
import functools

import jax
import jax.numpy as jnp
from jax import lax
from jax.experimental import pallas as pl
from jax.experimental.pallas import tpu as pltpu
from jax.sharding import PartitionSpec as P

N = 20480
MESH = pl.DeviceIdType.MESH
LAG = 2
CHUNKS = 16
DEEPEST = 5
STEPS = CHUNKS + LAG * DEEPEST
TREE = {
    (0, 0): (0, (0,)),
    (1, 0): (1, (0, 1, 3)),
    (1, 3): (2, (0, 2, 3)),
    (1, 1): (2, (2,)),
    (2, 0): (2, (0, 1)),
    (2, 3): (3, (0,)),
    (1, 2): (3, (2,)),
    (0, 1): (3, ()),
    (0, 3): (3, ()),
    (2, 1): (3, (0, 1)),
    (3, 0): (3, ()),
    (2, 2): (4, (0,)),
    (0, 2): (4, ()),
    (3, 1): (4, ()),
    (3, 3): (4, ()),
    (3, 2): (5, ()),
}


def look_up(index, table):
    found = jnp.int32(0)
    for key, value in enumerate(table):
        found = jnp.where(index == key, jnp.int32(value), found)
    return found


def gather_kernel(
    block_ref, trailing_ref,
    t_ref, acc_ref, a_last, b_last, sum_ref,
    at, b32, a_cat, b_cat, weave, sq_mine, sq_got,
    load_sem, trailing_sem, copy_sem, y_send, y_recv, d_send, d_recv,
    tree_send, tree_recv, sq_send, sq_recv,
):
    row = lax.axis_index("row")
    col = lax.axis_index("col")
    x, z = row // 4, row % 4
    y, core = col // 2, col % 2

    def device(dx=0, dy=0, dz=0):
        return ((x + dx) % 4 * 4 + (z + dz) % 4, (y + dy) % 4 * 2 + core)

    partner = (row, y * 2 + 1 - core)
    y_up, y_down = device(dy=1), device(dy=3)
    around = (device(dx=1), device(dz=1), device(dx=3), device(dz=3))

    trailing_copy = pltpu.make_async_copy(trailing_ref, t_ref, trailing_sem)
    own = pl.multiple_of(col * 64, 64)
    load = pltpu.make_async_copy(block_ref, at.at[pl.ds(own, 64)], load_sem)
    load.start()
    barrier = pltpu.get_barrier_semaphore()
    for peer in (partner, y_up, y_down, *around):
        pl.semaphore_signal(barrier, inc=1, device_id=peer, device_id_type=MESH)
    load.wait()
    pl.semaphore_wait(barrier, 7)

    def half(y_off, same, h):
        owner = (y + y_off) % 4 * 2 + (core if same else 1 - core)
        return pl.ds(pl.multiple_of(owner * 64 + 32 * h, 32), 32)

    def send(rows, send_sem, recv_sem, to):
        return pltpu.make_async_remote_copy(
            src_ref=at.at[rows], dst_ref=at.at[rows], send_sem=send_sem, recv_sem=recv_sem,
            device_id=to, device_id_type=MESH,
        )

    for h in (0, 1):
        send(half(0, True, h), y_send.at[0], y_recv.at[2 + h], y_up).start()
        send(half(0, True, h), y_send.at[1], y_recv.at[h], y_down).start()
        send(half(0, True, h), d_send, d_recv.at[h], partner).start()

    trailing_copy.start()
    value = at[pl.ds(own, 64), :]
    square = jnp.sum((value * value).reshape(8, 8, 1280), axis=0)
    total = square[:, 0:128]
    for tile in range(1, 10):
        total = total + square[:, 128 * tile : 128 * tile + 128]
    sq_mine[0] = total

    def got_y(index, y_off, h):
        send(half(y_off, True, h), y_send.at[0], y_recv.at[index], y_up).wait_recv()

    def got_d(index, y_off, h):
        send(half(y_off, False, h), d_send, d_recv.at[index], partner).wait_recv()

    def over(index, y_off, h):
        send(half(y_off, True, h), d_send, d_recv.at[index], partner).start()

    def quarter(rel):
        return pl.ds(pl.multiple_of((y + rel) % 4 * 128, 128), 128)

    roots = []
    plans = []
    for p in range(2):
        u = (x - (y // 2 + 2 * p)) % 4
        v = (z - (y % 2 * 2 + core)) % 4
        roots.append((u == 0) & (v == 0))
        for t in range(4):
            cu, cv = ((u, v), (v, (4 - u) % 4), ((4 - u) % 4, (4 - v) % 4), ((4 - v) % 4, u))[t]
            table = [TREE[i // 4, i % 4] for i in range(16)]
            code = look_up(cu * 4 + cv, [d + 8 * sum(1 << k for k in kids) for d, kids in table])
            plans.append((p, t, code % 8, code // 8))

    def own_copy(p, rel):
        rows = quarter(rel)
        return pltpu.make_async_copy(at.at[rows], b32.at[p, rows], copy_sem.at[p, rel])

    def convert(rel, first=0, last=10):
        if first == 0:
            for p in range(2):
                @pl.when(roots[p])
                def _():
                    own_copy(p, rel).wait()
        rows = quarter(rel)
        a_to, b_to, base = (a_last, b_last, 0) if rel == 2 else (a_cat, b_cat, 384 * (0, 1, None, 2)[rel])

        def split(value):
            high = value.astype(jnp.bfloat16)
            return high, (value - high.astype(jnp.float32)).astype(jnp.bfloat16)

        @pl.loop(first, last, unroll=2)
        def _(n):
            lanes = pl.ds(pl.multiple_of(n * 128, 128), 128)
            high, low = split(at[rows, lanes].T)
            for k, part in enumerate((high, high, low)):
                a_to[lanes, base + 128 * k : base + 128 * k + 128] = part
            for p in range(2):
                weave[n % 2, pl.ds(p, 128, stride=2), :] = b32[p, rows, lanes].T
            wide = pl.ds(pl.multiple_of(n * 256, 256), 256)
            high, low = split(weave[n % 2])
            for k, part in enumerate((high, low, high)):
                b_to[wide, base + 128 * k : base + 128 * k + 128] = part

    def product(b, start, stop):
        rows, cols = slice(256 * b, 1280), slice(512 * b, 512 * b + 512)
        return lax.dot_general(
            a_cat[rows, start:stop], b_cat[cols, start:stop],
            (((1,), (1,)), ((), ())), preferred_element_type=jnp.float32,
        )

    def sq_peer(e):
        flip_x = jnp.where(e == 3, x + 1 - 2 * (x % 2), jnp.where(e == 4, 3 - x, x))
        flip_z = jnp.where(e == 5, z + 1 - 2 * (z % 2), jnp.where(e == 6, 3 - z, z))
        flip_y = jnp.where(e == 1, y + 1 - 2 * (y % 2), jnp.where(e == 2, 3 - y, y))
        flip_core = jnp.where(e == 0, 1 - core, core)
        return (flip_x * 4 + flip_z, flip_y * 2 + flip_core)

    def sq_copy(e):
        return pltpu.make_async_remote_copy(
            src_ref=sq_mine.at[e], dst_ref=sq_got.at[e], send_sem=sq_send.at[e], recv_sem=sq_recv.at[e],
            device_id=sq_peer(e), device_id_type=MESH,
        )

    def chunk_rows(c, t):
        group, low = c // 4, c % 2
        middle = (group == 1) | (group == 2)
        h = jnp.where(middle, group - 1, low)
        y_off = jnp.where(middle, 1 + 2 * low, jnp.where(group == 0, 0, 2))
        owner = (y + y_off) % 4 * 2 + (core + c // 2) % 2
        return pl.ds(pl.multiple_of(owner * 64 + 32 * h + 8 * t, 8), 8)

    @pl.loop(0, STEPS)
    def _(s):
        @pl.when(s == 2)
        def _():
            got_d(0, 0, 0)
            got_d(1, 0, 1)

        @pl.when(s == 4)
        def _():
            got_y(2, 3, 0)
            send(half(3, True, 0), y_send.at[2], y_recv.at[4], y_up).start()
            over(4, 3, 0)
            got_y(0, 1, 0)
            over(2, 1, 0)
            for p in range(2):
                @pl.when(roots[p])
                def _():
                    own_copy(p, 0).start()

        @pl.when(s == 6)
        def _():
            got_d(2, 1, 0)
            got_d(4, 3, 0)

        @pl.when(s == 8)
        def _():
            got_y(1, 1, 1)
            send(half(1, True, 1), y_send.at[3], y_recv.at[5], y_down).start()
            over(3, 1, 1)
            got_y(3, 3, 1)
            over(5, 3, 1)

        @pl.when(s == 10)
        def _():
            got_d(3, 1, 1)
            got_d(5, 3, 1)
            for p in range(2):
                @pl.when(roots[p])
                def _():
                    own_copy(p, 1).start()
                    own_copy(p, 3).start()

        @pl.when(s == 12)
        def _():
            got_y(4, 2, 0)
            over(6, 2, 0)
            got_y(5, 2, 1)
            over(7, 2, 1)

        @pl.when(s == 14)
        def _():
            got_d(6, 2, 0)
            got_d(7, 2, 1)
            for p in range(2):
                @pl.when(roots[p])
                def _():
                    own_copy(p, 2).start()

        for p, t, depth, kids in plans:
            c = s - LAG * depth
            live = (c >= 0) & (c < CHUNKS)
            rows = chunk_rows(c, t)

            def forward(src, d, c=c, rows=rows, p=p, t=t):
                return pltpu.make_async_remote_copy(
                    src_ref=src, dst_ref=b32.at[p, rows],
                    send_sem=tree_send.at[p, t, d], recv_sem=tree_recv.at[p, t, c],
                    device_id=around[(d + t) % 4], device_id_type=MESH,
                )

            @pl.when(live & (depth == 0))
            def _():
                forward(at.at[rows], 0).start()

            @pl.when(live & (depth > 0))
            def _():
                forward(b32.at[p, rows], 0).wait_recv()
                for d in range(4):
                    @pl.when(kids // (1 << d) % 2 == 1)
                    def _():
                        forward(b32.at[p, rows], d).start()

        @pl.when((s % 3 == 0) & (s < 21))
        def _():
            sq_copy(s // 3).start()

        @pl.when((s % 3 == 2) & (s < 21))
        def _():
            e = s // 3
            sq_copy(e).wait_recv()
            sq_mine[e + 1] = sq_mine[e] + sq_got[e]

        ready = 3 + LAG * DEEPEST
        for k in range(5):
            @pl.when(s == ready + k)
            def _():
                convert(0, 2 * k, 2 * k + 2)

            @pl.when(s == ready + 5 + k // 2)
            def _():
                acc_ref[256 * k : 1280, 512 * k : 512 * k + 512] = product(k, 0, 384)

        @pl.when(s == ready + 8)
        def _():
            convert(1)

        @pl.when(s == ready + 9)
        def _():
            convert(3)

        @pl.when(s == ready + 10)
        def _():
            for k in (0, 1):
                acc_ref[256 * k : 1280, 512 * k : 512 * k + 512] += product(k, 384, 1152)

        @pl.when(s == ready + 11)
        def _():
            for k in (2, 3, 4):
                acc_ref[256 * k : 1280, 512 * k : 512 * k + 512] += product(k, 384, 1152)


    convert(2)
    sum_ref[...] = sq_mine[7]

    def sent(sem, rows):
        return pltpu.make_async_remote_copy(
            src_ref=at.at[pl.ds(0, rows)], dst_ref=at.at[pl.ds(0, rows)], send_sem=sem, recv_sem=sem,
            device_id=partner, device_id_type=MESH,
        ).wait_send()

    for p, t, depth, kids in plans:
        for d in range(4):
            @pl.when(kids // (1 << d) % 2 == 1)
            def _():
                sent(tree_send.at[p, t, d], CHUNKS * 8)

    sent(y_send.at[0], 64)
    sent(y_send.at[1], 64)
    sent(y_send.at[2], 32)
    sent(y_send.at[3], 32)
    sent(d_send, 256)

    @pl.loop(0, 7)
    def _(e):
        sq_copy(e).wait_send()

    trailing_copy.wait()


def update_kernel(t_ref, acc_ref, a_ref, b_ref, sum_ref, out_ref, stage, upper_sem, lower_sem):
    row = lax.axis_index("row")
    col = lax.axis_index("col")

    def upper(a):
        where = (pl.ds(256 * a, 256), pl.ds(512 * (a + 1), 2560 - 512 * (a + 1)))
        return pltpu.make_async_copy(t_ref.at[where], out_ref.at[where], upper_sem.at[a])

    def lower(b):
        where = (pl.ds(256 * b, 1280 - 256 * b), pl.ds(512 * b, 512))
        return pltpu.make_async_copy(stage.at[where], out_ref.at[where], lower_sem.at[b])

    for a in range(4):
        upper(a).start()
    squares = jnp.full((8, 512), jnp.sum(sum_ref[...]), jnp.float32)
    factor = (0.8 * jnp.sqrt(jnp.float32(N)) / jnp.sqrt(squares + 1e-6))[0:1, :]
    i = lax.broadcasted_iota(jnp.int32, (256, 512), 0)
    j = lax.broadcasted_iota(jnp.int32, (256, 512), 1)
    for b in range(5):
        cols = slice(512 * b, 512 * b + 512)
        update = acc_ref[256 * b : 1280, cols] + lax.dot_general(
            a_ref[256 * b : 1280, :], b_ref[cols, :],
            (((1,), (1,)), ((), ())), preferred_element_type=jnp.float32,
        )
        edge = slice(256 * b, 256 * b + 256)
        below = (256 * b + i) * 16 + row >= (512 * b + j) * 8 + col
        stage[edge, cols] = t_ref[edge, cols] - factor * jnp.where(below, update[0:256], 0.0)
        if b < 4:
            rest = slice(256 * b + 256, 1280)
            stage[rest, cols] = t_ref[rest, cols] - factor * update[256:]
        lower(b).start()
    for a in range(4):
        upper(a).wait()
    for b in range(5):
        lower(b).wait()


def on_device(panel_block, trailing):
    bf16 = jnp.bfloat16
    f32 = jnp.float32
    dma = pltpu.SemaphoreType.DMA
    anywhere = pl.BlockSpec(memory_space=pl.ANY)
    in_hbm = functools.partial(pltpu.with_memory_space_constraint, memory_space=pltpu.HBM)
    vmem = pl.BlockSpec(memory_space=pltpu.VMEM)
    gathered = pl.pallas_call(
        gather_kernel,
        out_shape=(
            pltpu.VMEM((1280, 2560), f32),
            pltpu.VMEM((1280, 2560), f32),
            pltpu.VMEM((1280, 384), bf16),
            pltpu.VMEM((2560, 384), bf16),
            pltpu.VMEM((8, 128), f32),
        ),
        in_specs=[anywhere, anywhere],
        out_specs=[vmem] * 5,
        scratch_shapes=[
            pltpu.VMEM((512, 1280), f32),
            pltpu.VMEM((2, 512, 1280), f32),
            pltpu.VMEM((1280, 1152), bf16),
            pltpu.VMEM((2560, 1152), bf16),
            pltpu.VMEM((2, 256, 128), f32),
            pltpu.VMEM((8, 8, 128), f32),
            pltpu.VMEM((7, 8, 128), f32),
            dma(()), dma(()), dma((2, 4)), dma((4,)), dma((6,)), dma(()), dma((8,)),
            dma((2, 4, 4)), dma((2, 4, CHUNKS)), dma((7,)), dma((7,)),
        ],
        compiler_params=pltpu.CompilerParams(
            collective_id=0, has_side_effects=True, vmem_limit_bytes=24 * 1024 * 1024
        ),
        name="gather",
    )(in_hbm(panel_block.T), in_hbm(trailing))
    return pl.pallas_call(
        update_kernel,
        out_shape=jax.ShapeDtypeStruct((1280, 2560), f32),
        in_specs=[vmem] * 5,
        out_specs=anywhere,
        scratch_shapes=[pltpu.VMEM((1280, 2560), f32), dma((4,)), dma((5,))],
        compiler_params=pltpu.CompilerParams(vmem_limit_bytes=24 * 1024 * 1024),
        name="update",
    )(*gathered)


def solution(mesh):
    return jax.shard_map(
        on_device,
        mesh=mesh,
        in_specs=(P("row", "col"), P("row", "col")),
        out_specs=P("row", "col"),
        check_vma=False,
    )
```

```python
import functools

import jax
import jax.numpy as jnp
from jax import lax
from jax.experimental import pallas as pl
from jax.experimental.pallas import tpu as pltpu
from jax.sharding import PartitionSpec as P

N = 20480
MESH = pl.DeviceIdType.MESH
LAG = 2
CHUNKS = 16
INNER = 4
STEPS = CHUNKS + LAG * INNER
TREE = {
    (0, 0): (0, (0,)),
    (1, 0): (1, (0, 1, 3)),
    (1, 3): (2, (0, 2, 3)),
    (1, 1): (2, (2,)),
    (2, 0): (2, (0, 1)),
    (2, 3): (3, (0,)),
    (1, 2): (3, (2,)),
    (0, 1): (3, ()),
    (0, 3): (3, ()),
    (2, 1): (3, (0, 1)),
    (3, 0): (3, ()),
    (2, 2): (4, (0,)),
    (0, 2): (4, ()),
    (3, 1): (4, ()),
    (3, 3): (4, ()),
    (3, 2): (5, ()),
}


def encode(u, v):
    depth, kids = TREE[u, v]
    step = ((1, 0), (0, 1), (3, 0), (0, 3))
    ends = [k for k in kids if not TREE[(u + step[k][0]) % 4, (v + step[k][1]) % 4][1]]
    return depth + 8 * sum(1 << k for k in kids) + 128 * sum(1 << k for k in ends)


def look_up(index, table):
    found = jnp.int32(0)
    for key, value in enumerate(table):
        found = jnp.where(index == key, jnp.int32(value), found)
    return found


def gather_kernel(
    block_ref, trailing_ref,
    t_ref, acc_ref, a_last, b_last, sum_ref,
    at, b32, a_cat, b_cat, weave, sq_mine, sq_got,
    load_sem, trailing_sem, copy_sem, y_send, y_recv, d_send, d_recv,
    tree_send, tree_recv, sq_send, sq_recv,
):
    row = lax.axis_index("row")
    col = lax.axis_index("col")
    x, z = row // 4, row % 4
    y, core = col // 2, col % 2

    def device(dx=0, dy=0, dz=0):
        return ((x + dx) % 4 * 4 + (z + dz) % 4, (y + dy) % 4 * 2 + core)

    partner = (row, y * 2 + 1 - core)
    y_up, y_down = device(dy=1), device(dy=3)
    around = (device(dx=1), device(dz=1), device(dx=3), device(dz=3))

    trailing_copy = pltpu.make_async_copy(trailing_ref, t_ref, trailing_sem)
    own = pl.multiple_of(col * 64, 64)
    load = pltpu.make_async_copy(block_ref, at.at[pl.ds(own, 64)], load_sem)
    load.start()
    barrier = pltpu.get_barrier_semaphore()
    for peer in (partner, y_up, y_down, *around):
        pl.semaphore_signal(barrier, inc=1, device_id=peer, device_id_type=MESH)
    load.wait()
    pl.semaphore_wait(barrier, 7)

    def half(y_off, same, h):
        owner = (y + y_off) % 4 * 2 + (core if same else 1 - core)
        return pl.ds(pl.multiple_of(owner * 64 + 32 * h, 32), 32)

    def send(rows, send_sem, recv_sem, to):
        return pltpu.make_async_remote_copy(
            src_ref=at.at[rows], dst_ref=at.at[rows], send_sem=send_sem, recv_sem=recv_sem,
            device_id=to, device_id_type=MESH,
        )

    for h in (0, 1):
        send(half(0, True, h), y_send.at[0], y_recv.at[2 + h], y_up).start()
        send(half(0, True, h), y_send.at[1], y_recv.at[h], y_down).start()
        send(half(0, True, h), d_send, d_recv.at[h], partner).start()

    trailing_copy.start()
    value = at[pl.ds(own, 64), :]
    square = jnp.sum((value * value).reshape(8, 8, 1280), axis=0)
    total = square[:, 0:128]
    for tile in range(1, 10):
        total = total + square[:, 128 * tile : 128 * tile + 128]
    sq_mine[0] = total

    def got_y(index, y_off, h):
        send(half(y_off, True, h), y_send.at[0], y_recv.at[index], y_up).wait_recv()

    def got_d(index, y_off, h):
        send(half(y_off, False, h), d_send, d_recv.at[index], partner).wait_recv()

    def over(index, y_off, h):
        send(half(y_off, True, h), d_send, d_recv.at[index], partner).start()

    def quarter(rel):
        return pl.ds(pl.multiple_of((y + rel) % 4 * 128, 128), 128)

    roots = []
    plans = []
    for p in range(2):
        u = (x - (y // 2 + 2 * p)) % 4
        v = (z - (y % 2 * 2 + core)) % 4
        roots.append((u == 0) & (v == 0))
        for t in range(4):
            cu, cv = ((u, v), (v, (4 - u) % 4), ((4 - u) % 4, (4 - v) % 4), ((4 - v) % 4, u))[t]
            code = look_up(cu * 4 + cv, [encode(i // 4, i % 4) for i in range(16)])
            plans.append((p, t, code % 8, code // 8 % 16, code // 128))

    def own_copy(p, rel):
        rows = quarter(rel)
        return pltpu.make_async_copy(at.at[rows], b32.at[p, rows], copy_sem.at[p, rel])

    def convert(rel, first=0, last=10):
        if first == 0:
            for p in range(2):
                @pl.when(roots[p])
                def _():
                    own_copy(p, rel).wait()
        rows = quarter(rel)
        a_to, b_to, base = (a_last, b_last, 0) if rel == 2 else (a_cat, b_cat, 384 * (0, 1, None, 2)[rel])

        def split(value):
            high = value.astype(jnp.bfloat16)
            return high, (value - high.astype(jnp.float32)).astype(jnp.bfloat16)

        @pl.loop(first, last, unroll=2)
        def _(n):
            lanes = pl.ds(pl.multiple_of(n * 128, 128), 128)
            high, low = split(at[rows, lanes].T)
            for k, part in enumerate((high, high, low)):
                a_to[lanes, base + 128 * k : base + 128 * k + 128] = part
            for p in range(2):
                weave[n % 2, pl.ds(p, 128, stride=2), :] = b32[p, rows, lanes].T
            wide = pl.ds(pl.multiple_of(n * 256, 256), 256)
            high, low = split(weave[n % 2])
            for k, part in enumerate((high, low, high)):
                b_to[wide, base + 128 * k : base + 128 * k + 128] = part

    def product(b, start, stop):
        rows, cols = slice(256 * b, 1280), slice(512 * b, 512 * b + 512)
        return lax.dot_general(
            a_cat[rows, start:stop], b_cat[cols, start:stop],
            (((1,), (1,)), ((), ())), preferred_element_type=jnp.float32,
        )

    def multiply(start, stop, *blocks):
        for k in blocks:
            where = (slice(256 * k, 1280), slice(512 * k, 512 * k + 512))
            if start == 0:
                acc_ref[where] = product(k, start, stop)
            else:
                acc_ref[where] += product(k, start, stop)

    def ended(group):
        rows = pl.ds(0, (32, 64, 32)[group])
        for p, t, depth, kids, ends in plans:
            @pl.when(kids == 0)
            def _():
                pltpu.make_async_copy(b32.at[p, rows], b32.at[p, rows], tree_recv.at[p, t, 16 + group]).wait()

    def sq_peer(e):
        flip_x = jnp.where(e == 3, x + 1 - 2 * (x % 2), jnp.where(e == 4, 3 - x, x))
        flip_z = jnp.where(e == 5, z + 1 - 2 * (z % 2), jnp.where(e == 6, 3 - z, z))
        flip_y = jnp.where(e == 1, y + 1 - 2 * (y % 2), jnp.where(e == 2, 3 - y, y))
        flip_core = jnp.where(e == 0, 1 - core, core)
        return (flip_x * 4 + flip_z, flip_y * 2 + flip_core)

    def sq_copy(e):
        return pltpu.make_async_remote_copy(
            src_ref=sq_mine.at[e], dst_ref=sq_got.at[e], send_sem=sq_send.at[e], recv_sem=sq_recv.at[e],
            device_id=sq_peer(e), device_id_type=MESH,
        )

    def chunk_rows(c, t):
        group, low = c // 4, c % 2
        middle = (group == 1) | (group == 2)
        h = jnp.where(middle, group - 1, low)
        y_off = jnp.where(middle, 1 + 2 * low, jnp.where(group == 0, 0, 2))
        owner = (y + y_off) % 4 * 2 + (core + c // 2) % 2
        return pl.ds(pl.multiple_of(owner * 64 + 32 * h + 8 * t, 8), 8)

    @pl.loop(0, STEPS)
    def _(s):
        @pl.when(s == 2)
        def _():
            got_d(0, 0, 0)
            got_d(1, 0, 1)

        @pl.when(s == 4)
        def _():
            got_y(2, 3, 0)
            send(half(3, True, 0), y_send.at[2], y_recv.at[4], y_up).start()
            over(4, 3, 0)
            got_y(0, 1, 0)
            over(2, 1, 0)
            for p in range(2):
                @pl.when(roots[p])
                def _():
                    own_copy(p, 0).start()

        @pl.when(s == 6)
        def _():
            got_d(2, 1, 0)
            got_d(4, 3, 0)

        @pl.when(s == 8)
        def _():
            got_y(1, 1, 1)
            send(half(1, True, 1), y_send.at[3], y_recv.at[5], y_down).start()
            over(3, 1, 1)
            got_y(3, 3, 1)
            over(5, 3, 1)

        @pl.when(s == 10)
        def _():
            got_d(3, 1, 1)
            got_d(5, 3, 1)
            for p in range(2):
                @pl.when(roots[p])
                def _():
                    own_copy(p, 1).start()
                    own_copy(p, 3).start()

        @pl.when(s == 12)
        def _():
            got_y(4, 2, 0)
            over(6, 2, 0)
            got_y(5, 2, 1)
            over(7, 2, 1)

        @pl.when(s == 14)
        def _():
            got_d(6, 2, 0)
            got_d(7, 2, 1)
            for p in range(2):
                @pl.when(roots[p])
                def _():
                    own_copy(p, 2).start()

        for p, t, depth, kids, ends in plans:
            c = s - LAG * depth
            live = (c >= 0) & (c < CHUNKS)
            rows = chunk_rows(c, t)
            late = 16 + jnp.where(c >= 4, 1, 0) + jnp.where(c >= 12, 1, 0) - c

            def forward(src, d, c=c, rows=rows, p=p, t=t, late=late, ends=ends):
                return pltpu.make_async_remote_copy(
                    src_ref=src, dst_ref=b32.at[p, rows],
                    send_sem=tree_send.at[p, t, d], recv_sem=tree_recv.at[p, t, c + late * (ends // (1 << d) % 2)],
                    device_id=around[(d + t) % 4], device_id_type=MESH,
                )

            @pl.when(live & (depth == 0))
            def _():
                forward(at.at[rows], 0).start()

            @pl.when(live & (depth > 0) & (kids > 0))
            def _():
                pltpu.make_async_copy(b32.at[p, rows], b32.at[p, rows], tree_recv.at[p, t, c]).wait()
                for d in range(4):
                    @pl.when(kids // (1 << d) % 2 == 1)
                    def _():
                        forward(b32.at[p, rows], d).start()

        @pl.when((s % 3 == 0) & (s < 21))
        def _():
            sq_copy(s // 3).start()

        @pl.when((s % 3 == 2) & (s < 21))
        def _():
            e = s // 3
            sq_copy(e).wait_recv()
            sq_mine[e + 1] = sq_mine[e] + sq_got[e]

        ready = 3 + LAG * (INNER + 1)

        @pl.when(s == ready)
        def _():
            ended(0)

        for k in range(5):
            @pl.when(s == ready + k)
            def _():
                convert(0, 2 * k, 2 * k + 2)

            @pl.when(s == ready + 5 + k // 2)
            def _():
                multiply(0, 384, k)

        @pl.when(s == ready + 8)
        def _():
            ended(1)
            convert(1)

        @pl.when(s == ready + 9)
        def _():
            convert(3)

        @pl.when(s == ready + 10)
        def _():
            multiply(384, 1152, 0, 1)

    multiply(384, 1152, 2, 3, 4)
    ended(2)
    convert(2)
    sum_ref[...] = sq_mine[7]

    def sent(sem, rows):
        return pltpu.make_async_remote_copy(
            src_ref=at.at[pl.ds(0, rows)], dst_ref=at.at[pl.ds(0, rows)], send_sem=sem, recv_sem=sem,
            device_id=partner, device_id_type=MESH,
        ).wait_send()

    for p, t, depth, kids, ends in plans:
        for d in range(4):
            @pl.when(kids // (1 << d) % 2 == 1)
            def _():
                sent(tree_send.at[p, t, d], CHUNKS * 8)

    sent(y_send.at[0], 64)
    sent(y_send.at[1], 64)
    sent(y_send.at[2], 32)
    sent(y_send.at[3], 32)
    sent(d_send, 256)

    @pl.loop(0, 7)
    def _(e):
        sq_copy(e).wait_send()

    trailing_copy.wait()


def update_kernel(t_ref, acc_ref, a_ref, b_ref, sum_ref, out_ref, stage, upper_sem, lower_sem):
    row = lax.axis_index("row")
    col = lax.axis_index("col")

    def upper(a):
        where = (pl.ds(256 * a, 256), pl.ds(512 * (a + 1), 2560 - 512 * (a + 1)))
        return pltpu.make_async_copy(t_ref.at[where], out_ref.at[where], upper_sem.at[a])

    def lower(b):
        where = (pl.ds(256 * b, 1280 - 256 * b), pl.ds(512 * b, 512))
        return pltpu.make_async_copy(stage.at[where], out_ref.at[where], lower_sem.at[b])

    for a in range(4):
        upper(a).start()
    squares = jnp.full((8, 512), jnp.sum(sum_ref[...]), jnp.float32)
    factor = (0.8 * jnp.sqrt(jnp.float32(N)) / jnp.sqrt(squares + 1e-6))[0:1, :]
    i = lax.broadcasted_iota(jnp.int32, (256, 512), 0)
    j = lax.broadcasted_iota(jnp.int32, (256, 512), 1)
    for b in range(5):
        cols = slice(512 * b, 512 * b + 512)
        update = acc_ref[256 * b : 1280, cols] + lax.dot_general(
            a_ref[256 * b : 1280, :], b_ref[cols, :],
            (((1,), (1,)), ((), ())), preferred_element_type=jnp.float32,
        )
        edge = slice(256 * b, 256 * b + 256)
        below = (256 * b + i) * 16 + row >= (512 * b + j) * 8 + col
        stage[edge, cols] = t_ref[edge, cols] - factor * jnp.where(below, update[0:256], 0.0)
        if b < 4:
            rest = slice(256 * b + 256, 1280)
            stage[rest, cols] = t_ref[rest, cols] - factor * update[256:]
        lower(b).start()
    for a in range(4):
        upper(a).wait()
    for b in range(5):
        lower(b).wait()


def on_device(panel_block, trailing):
    bf16 = jnp.bfloat16
    f32 = jnp.float32
    dma = pltpu.SemaphoreType.DMA
    anywhere = pl.BlockSpec(memory_space=pl.ANY)
    in_hbm = functools.partial(pltpu.with_memory_space_constraint, memory_space=pltpu.HBM)
    vmem = pl.BlockSpec(memory_space=pltpu.VMEM)
    gathered = pl.pallas_call(
        gather_kernel,
        out_shape=(
            pltpu.VMEM((1280, 2560), f32),
            pltpu.VMEM((1280, 2560), f32),
            pltpu.VMEM((1280, 384), bf16),
            pltpu.VMEM((2560, 384), bf16),
            pltpu.VMEM((8, 128), f32),
        ),
        in_specs=[anywhere, anywhere],
        out_specs=[vmem] * 5,
        scratch_shapes=[
            pltpu.VMEM((512, 1280), f32),
            pltpu.VMEM((2, 512, 1280), f32),
            pltpu.VMEM((1280, 1152), bf16),
            pltpu.VMEM((2560, 1152), bf16),
            pltpu.VMEM((2, 256, 128), f32),
            pltpu.VMEM((8, 8, 128), f32),
            pltpu.VMEM((7, 8, 128), f32),
            dma(()), dma(()), dma((2, 4)), dma((4,)), dma((6,)), dma(()), dma((8,)),
            dma((2, 4, 4)), dma((2, 4, CHUNKS + 3)), dma((7,)), dma((7,)),
        ],
        compiler_params=pltpu.CompilerParams(
            collective_id=0, has_side_effects=True, vmem_limit_bytes=24 * 1024 * 1024
        ),
        name="gather",
    )(in_hbm(panel_block.T), in_hbm(trailing))
    return pl.pallas_call(
        update_kernel,
        out_shape=jax.ShapeDtypeStruct((1280, 2560), f32),
        in_specs=[vmem] * 5,
        out_specs=anywhere,
        scratch_shapes=[pltpu.VMEM((1280, 2560), f32), dma((4,)), dma((5,))],
        compiler_params=pltpu.CompilerParams(vmem_limit_bytes=24 * 1024 * 1024),
        name="update",
    )(*gathered)


def solution(mesh):
    return jax.shard_map(
        on_device,
        mesh=mesh,
        in_specs=(P("row", "col"), P("row", "col")),
        out_specs=P("row", "col"),
        check_vma=False,
    )
```

```python
import functools

import jax
import jax.numpy as jnp
from jax import lax
from jax.experimental import pallas as pl
from jax.experimental.pallas import tpu as pltpu
from jax.sharding import PartitionSpec as P

N = 20480
MESH = pl.DeviceIdType.MESH
LAG = 2
CHUNKS = 16
INNER = 4
STEPS = CHUNKS + LAG * INNER
TREE = {
    (0, 0): (0, (0,)),
    (1, 0): (1, (0, 1, 3)),
    (1, 3): (2, (0, 2, 3)),
    (1, 1): (2, (2,)),
    (2, 0): (2, (0, 1)),
    (2, 3): (3, (0,)),
    (1, 2): (3, (2,)),
    (0, 1): (3, ()),
    (0, 3): (3, ()),
    (2, 1): (3, (0, 1)),
    (3, 0): (3, ()),
    (2, 2): (4, (0,)),
    (0, 2): (4, ()),
    (3, 1): (4, ()),
    (3, 3): (4, ()),
    (3, 2): (5, ()),
}


def encode(u, v):
    depth, kids = TREE[u, v]
    step = ((1, 0), (0, 1), (3, 0), (0, 3))
    ends = [k for k in kids if not TREE[(u + step[k][0]) % 4, (v + step[k][1]) % 4][1]]
    if not kids:
        depth = 63
    return depth + 64 * sum(1 << k for k in kids) + 1024 * sum(1 << k for k in ends)


def look_up(index, table):
    found = jnp.int32(0)
    for key, value in enumerate(table):
        found = jnp.where(index == key, jnp.int32(value), found)
    return found


def gather_kernel(
    block_ref, trailing_ref,
    t_ref, acc_ref, a_last, b_last, sum_ref,
    at, b32, a_cat, b_cat, weave, sq_mine, sq_got,
    load_sem, trailing_sem, copy_sem, y_send, y_recv, d_send, d_recv,
    tree_send, tree_recv, sq_send, sq_recv,
):
    row = lax.axis_index("row")
    col = lax.axis_index("col")
    x, z = row // 4, row % 4
    y, core = col // 2, col % 2

    def device(dx=0, dy=0, dz=0):
        return ((x + dx) % 4 * 4 + (z + dz) % 4, (y + dy) % 4 * 2 + core)

    partner = (row, y * 2 + 1 - core)
    y_up, y_down = device(dy=1), device(dy=3)
    around = (device(dx=1), device(dz=1), device(dx=3), device(dz=3))

    trailing_copy = pltpu.make_async_copy(trailing_ref, t_ref, trailing_sem)
    own = pl.multiple_of(col * 64, 64)
    load = pltpu.make_async_copy(block_ref, at.at[pl.ds(own, 64)], load_sem)
    load.start()
    barrier = pltpu.get_barrier_semaphore()
    for peer in (partner, y_up, y_down, *around):
        pl.semaphore_signal(barrier, inc=1, device_id=peer, device_id_type=MESH)
    load.wait()
    pl.semaphore_wait(barrier, 7)

    def half(y_off, same, h):
        owner = (y + y_off) % 4 * 2 + (core if same else 1 - core)
        return pl.ds(pl.multiple_of(owner * 64 + 32 * h, 32), 32)

    def send(rows, send_sem, recv_sem, to):
        return pltpu.make_async_remote_copy(
            src_ref=at.at[rows], dst_ref=at.at[rows], send_sem=send_sem, recv_sem=recv_sem,
            device_id=to, device_id_type=MESH,
        )

    for h in (0, 1):
        send(half(0, True, h), y_send.at[0], y_recv.at[2 + h], y_up).start()
        send(half(0, True, h), y_send.at[1], y_recv.at[h], y_down).start()
        send(half(0, True, h), d_send, d_recv.at[h], partner).start()

    trailing_copy.start()
    value = at[pl.ds(own, 64), :]
    square = jnp.sum((value * value).reshape(8, 8, 1280), axis=0)
    total = square[:, 0:128]
    for tile in range(1, 10):
        total = total + square[:, 128 * tile : 128 * tile + 128]
    sq_mine[0] = total

    def got_y(index, y_off, h):
        send(half(y_off, True, h), y_send.at[0], y_recv.at[index], y_up).wait_recv()

    def got_d(index, y_off, h):
        send(half(y_off, False, h), d_send, d_recv.at[index], partner).wait_recv()

    def over(index, y_off, h):
        send(half(y_off, True, h), d_send, d_recv.at[index], partner).start()

    def quarter(rel):
        return pl.ds(pl.multiple_of((y + rel) % 4 * 128, 128), 128)

    roots = []
    plans = []
    for p in range(2):
        u = (x - (y // 2 + 2 * p)) % 4
        v = (z - (y % 2 * 2 + core)) % 4
        roots.append((u == 0) & (v == 0))
        for t in range(4):
            cu, cv = ((u, v), (v, (4 - u) % 4), ((4 - u) % 4, (4 - v) % 4), ((4 - v) % 4, u))[t]
            code = look_up(cu * 4 + cv, [encode(i // 4, i % 4) for i in range(16)])
            plans.append((p, t, code % 64, code // 64 % 16, code // 1024))

    def own_copy(p, rel):
        rows = quarter(rel)
        return pltpu.make_async_copy(at.at[rows], b32.at[p, rows], copy_sem.at[p, rel])

    def convert(rel, first=0, last=10):
        if first == 0:
            for p in range(2):
                @pl.when(roots[p])
                def _():
                    own_copy(p, rel).wait()
        rows = quarter(rel)
        a_to, b_to, base = (a_last, b_last, 0) if rel == 2 else (a_cat, b_cat, 384 * (0, 1, None, 2)[rel])

        def split(value):
            high = value.astype(jnp.bfloat16)
            return high, (value - high.astype(jnp.float32)).astype(jnp.bfloat16)

        @pl.loop(first, last, unroll=2)
        def _(n):
            lanes = pl.ds(pl.multiple_of(n * 128, 128), 128)
            high, low = split(at[rows, lanes].T)
            for k, part in enumerate((high, high, low)):
                a_to[lanes, base + 128 * k : base + 128 * k + 128] = part
            for p in range(2):
                weave[n % 2, pl.ds(p, 128, stride=2), :] = b32[p, rows, lanes].T
            wide = pl.ds(pl.multiple_of(n * 256, 256), 256)
            high, low = split(weave[n % 2])
            for k, part in enumerate((high, low, high)):
                b_to[wide, base + 128 * k : base + 128 * k + 128] = part

    def product(b, start, stop):
        rows, cols = slice(256 * b, 1280), slice(512 * b, 512 * b + 512)
        return lax.dot_general(
            a_cat[rows, start:stop], b_cat[cols, start:stop],
            (((1,), (1,)), ((), ())), preferred_element_type=jnp.float32,
        )

    def multiply(start, stop, *blocks):
        for k in blocks:
            where = (slice(256 * k, 1280), slice(512 * k, 512 * k + 512))
            if start == 0:
                acc_ref[where] = product(k, start, stop)
            else:
                acc_ref[where] += product(k, start, stop)

    def ended(group):
        rows = pl.ds(0, (32, 64, 32)[group])
        for p, t, depth, kids, ends in plans:
            @pl.when(kids == 0)
            def _():
                pltpu.make_async_copy(b32.at[p, rows], b32.at[p, rows], tree_recv.at[p, t, 16 + group]).wait()

    def sq_peer(e):
        flip_x = jnp.where(e == 3, x + 1 - 2 * (x % 2), jnp.where(e == 4, 3 - x, x))
        flip_z = jnp.where(e == 5, z + 1 - 2 * (z % 2), jnp.where(e == 6, 3 - z, z))
        flip_y = jnp.where(e == 1, y + 1 - 2 * (y % 2), jnp.where(e == 2, 3 - y, y))
        flip_core = jnp.where(e == 0, 1 - core, core)
        return (flip_x * 4 + flip_z, flip_y * 2 + flip_core)

    def sq_copy(e):
        return pltpu.make_async_remote_copy(
            src_ref=sq_mine.at[e], dst_ref=sq_got.at[e], send_sem=sq_send.at[e], recv_sem=sq_recv.at[e],
            device_id=sq_peer(e), device_id_type=MESH,
        )

    def chunk_rows(c, t):
        group, low = c // 4, c % 2
        middle = (group == 1) | (group == 2)
        h = jnp.where(middle, group - 1, low)
        y_off = jnp.where(middle, 1 + 2 * low, jnp.where(group == 0, 0, 2))
        owner = (y + y_off) % 4 * 2 + (core + c // 2) % 2
        return pl.ds(pl.multiple_of(owner * 64 + 32 * h + 8 * t, 8), 8)

    @pl.loop(0, STEPS)
    def _(s):
        @pl.when(s == 2)
        def _():
            got_d(0, 0, 0)
            got_d(1, 0, 1)

        @pl.when(s == 4)
        def _():
            got_y(2, 3, 0)
            send(half(3, True, 0), y_send.at[2], y_recv.at[4], y_up).start()
            over(4, 3, 0)
            got_y(0, 1, 0)
            over(2, 1, 0)
            for p in range(2):
                @pl.when(roots[p])
                def _():
                    own_copy(p, 0).start()

        @pl.when(s == 6)
        def _():
            got_d(2, 1, 0)
            got_d(4, 3, 0)

        @pl.when(s == 8)
        def _():
            got_y(1, 1, 1)
            send(half(1, True, 1), y_send.at[3], y_recv.at[5], y_down).start()
            over(3, 1, 1)
            got_y(3, 3, 1)
            over(5, 3, 1)

        @pl.when(s == 10)
        def _():
            got_d(3, 1, 1)
            got_d(5, 3, 1)
            for p in range(2):
                @pl.when(roots[p])
                def _():
                    own_copy(p, 1).start()
                    own_copy(p, 3).start()

        @pl.when(s == 12)
        def _():
            got_y(4, 2, 0)
            over(6, 2, 0)
            got_y(5, 2, 1)
            over(7, 2, 1)

        @pl.when(s == 14)
        def _():
            got_d(6, 2, 0)
            got_d(7, 2, 1)
            for p in range(2):
                @pl.when(roots[p])
                def _():
                    own_copy(p, 2).start()

        for p, t, depth, kids, ends in plans:
            c = s - LAG * depth

            @pl.when((c >= 0) & (c < CHUNKS))
            def _():
                rows = chunk_rows(c, t)
                late = 16 + jnp.where(c >= 4, 1, 0) + jnp.where(c >= 12, 1, 0) - c

                def forward(src, d):
                    slot = c + late * (ends // (1 << d) % 2)
                    return pltpu.make_async_remote_copy(
                        src_ref=src, dst_ref=b32.at[p, rows],
                        send_sem=tree_send.at[p, t, d], recv_sem=tree_recv.at[p, t, slot],
                        device_id=around[(d + t) % 4], device_id_type=MESH,
                    )

                @pl.when(depth == 0)
                def _():
                    forward(at.at[rows], 0).start()

                @pl.when(depth > 0)
                def _():
                    pltpu.make_async_copy(b32.at[p, rows], b32.at[p, rows], tree_recv.at[p, t, c]).wait()
                    for d in range(4):
                        @pl.when(kids // (1 << d) % 2 == 1)
                        def _():
                            forward(b32.at[p, rows], d).start()

        @pl.when((s % 3 == 0) & (s < 21))
        def _():
            sq_copy(s // 3).start()

        @pl.when((s % 3 == 2) & (s < 21))
        def _():
            e = s // 3
            sq_copy(e).wait_recv()
            sq_mine[e + 1] = sq_mine[e] + sq_got[e]

        ready = 3 + LAG * (INNER + 1)

        @pl.when(s == ready)
        def _():
            ended(0)

        for k in range(5):
            @pl.when(s == ready + k)
            def _():
                convert(0, 2 * k, 2 * k + 2)

            @pl.when(s == ready + 5 + k // 2)
            def _():
                multiply(0, 384, k)

        @pl.when(s == ready + 8)
        def _():
            ended(1)
            convert(1)

        @pl.when(s == ready + 9)
        def _():
            convert(3)

        @pl.when(s == ready + 10)
        def _():
            multiply(384, 1152, 0, 1)

    multiply(384, 1152, 2, 3, 4)
    ended(2)
    convert(2)
    sum_ref[...] = sq_mine[7]

    def sent(sem, rows):
        return pltpu.make_async_remote_copy(
            src_ref=at.at[pl.ds(0, rows)], dst_ref=at.at[pl.ds(0, rows)], send_sem=sem, recv_sem=sem,
            device_id=partner, device_id_type=MESH,
        ).wait_send()

    for p, t, depth, kids, ends in plans:
        for d in range(4):
            @pl.when(kids // (1 << d) % 2 == 1)
            def _():
                sent(tree_send.at[p, t, d], CHUNKS * 8)

    sent(y_send.at[0], 64)
    sent(y_send.at[1], 64)
    sent(y_send.at[2], 32)
    sent(y_send.at[3], 32)
    sent(d_send, 256)

    @pl.loop(0, 7)
    def _(e):
        sq_copy(e).wait_send()

    trailing_copy.wait()


def update_kernel(t_ref, acc_ref, a_ref, b_ref, sum_ref, out_ref, stage, upper_sem, lower_sem):
    row = lax.axis_index("row")
    col = lax.axis_index("col")

    def upper(a):
        where = (pl.ds(256 * a, 256), pl.ds(512 * (a + 1), 2560 - 512 * (a + 1)))
        return pltpu.make_async_copy(t_ref.at[where], out_ref.at[where], upper_sem.at[a])

    def lower(b):
        where = (pl.ds(256 * b, 1280 - 256 * b), pl.ds(512 * b, 512))
        return pltpu.make_async_copy(stage.at[where], out_ref.at[where], lower_sem.at[b])

    for a in range(4):
        upper(a).start()
    squares = jnp.full((8, 512), jnp.sum(sum_ref[...]), jnp.float32)
    factor = (0.8 * jnp.sqrt(jnp.float32(N)) / jnp.sqrt(squares + 1e-6))[0:1, :]
    i = lax.broadcasted_iota(jnp.int32, (256, 512), 0)
    j = lax.broadcasted_iota(jnp.int32, (256, 512), 1)
    for b in range(5):
        cols = slice(512 * b, 512 * b + 512)
        update = acc_ref[256 * b : 1280, cols] + lax.dot_general(
            a_ref[256 * b : 1280, :], b_ref[cols, :],
            (((1,), (1,)), ((), ())), preferred_element_type=jnp.float32,
        )
        edge = slice(256 * b, 256 * b + 256)
        below = (256 * b + i) * 16 + row >= (512 * b + j) * 8 + col
        stage[edge, cols] = t_ref[edge, cols] - factor * jnp.where(below, update[0:256], 0.0)
        if b < 4:
            rest = slice(256 * b + 256, 1280)
            stage[rest, cols] = t_ref[rest, cols] - factor * update[256:]
        lower(b).start()
    for a in range(4):
        upper(a).wait()
    for b in range(5):
        lower(b).wait()


def on_device(panel_block, trailing):
    bf16 = jnp.bfloat16
    f32 = jnp.float32
    dma = pltpu.SemaphoreType.DMA
    anywhere = pl.BlockSpec(memory_space=pl.ANY)
    in_hbm = functools.partial(pltpu.with_memory_space_constraint, memory_space=pltpu.HBM)
    vmem = pl.BlockSpec(memory_space=pltpu.VMEM)
    gathered = pl.pallas_call(
        gather_kernel,
        out_shape=(
            pltpu.VMEM((1280, 2560), f32),
            pltpu.VMEM((1280, 2560), f32),
            pltpu.VMEM((1280, 384), bf16),
            pltpu.VMEM((2560, 384), bf16),
            pltpu.VMEM((8, 128), f32),
        ),
        in_specs=[anywhere, anywhere],
        out_specs=[vmem] * 5,
        scratch_shapes=[
            pltpu.VMEM((512, 1280), f32),
            pltpu.VMEM((2, 512, 1280), f32),
            pltpu.VMEM((1280, 1152), bf16),
            pltpu.VMEM((2560, 1152), bf16),
            pltpu.VMEM((2, 256, 128), f32),
            pltpu.VMEM((8, 8, 128), f32),
            pltpu.VMEM((7, 8, 128), f32),
            dma(()), dma(()), dma((2, 4)), dma((4,)), dma((6,)), dma(()), dma((8,)),
            dma((2, 4, 4)), dma((2, 4, CHUNKS + 3)), dma((7,)), dma((7,)),
        ],
        compiler_params=pltpu.CompilerParams(
            collective_id=0, has_side_effects=True, vmem_limit_bytes=24 * 1024 * 1024
        ),
        name="gather",
    )(in_hbm(panel_block.T), in_hbm(trailing))
    return pl.pallas_call(
        update_kernel,
        out_shape=jax.ShapeDtypeStruct((1280, 2560), f32),
        in_specs=[vmem] * 5,
        out_specs=anywhere,
        scratch_shapes=[pltpu.VMEM((1280, 2560), f32), dma((4,)), dma((5,))],
        compiler_params=pltpu.CompilerParams(vmem_limit_bytes=24 * 1024 * 1024),
        name="update",
    )(*gathered)


def solution(mesh):
    return jax.shard_map(
        on_device,
        mesh=mesh,
        in_specs=(P("row", "col"), P("row", "col")),
        out_specs=P("row", "col"),
        check_vma=False,
    )
```

```python
import functools

import jax
import jax.numpy as jnp
from jax import lax
from jax.experimental import pallas as pl
from jax.experimental.pallas import tpu as pltpu
from jax.sharding import PartitionSpec as P

N = 20480
MESH = pl.DeviceIdType.MESH
LAG = 2
CHUNKS = 16
INNER = 4
STEPS = CHUNKS + LAG * INNER
TREE = {
    (0, 0): (0, (0,)),
    (1, 0): (1, (0, 1, 3)),
    (1, 3): (2, (0, 2, 3)),
    (1, 1): (2, (2,)),
    (2, 0): (2, (0, 1)),
    (2, 3): (3, (0,)),
    (1, 2): (3, (2,)),
    (0, 1): (3, ()),
    (0, 3): (3, ()),
    (2, 1): (3, (0, 1)),
    (3, 0): (3, ()),
    (2, 2): (4, (0,)),
    (0, 2): (4, ()),
    (3, 1): (4, ()),
    (3, 3): (4, ()),
    (3, 2): (5, ()),
}


def encode(u, v):
    depth, kids = TREE[u, v]
    step = ((1, 0), (0, 1), (3, 0), (0, 3))
    ends = [k for k in kids if not TREE[(u + step[k][0]) % 4, (v + step[k][1]) % 4][1]]
    if not kids:
        depth = 63
    return depth + 64 * sum(1 << k for k in kids) + 1024 * sum(1 << k for k in ends)


def look_up(index, table):
    found = jnp.int32(0)
    for key, value in enumerate(table):
        found = jnp.where(index == key, jnp.int32(value), found)
    return found


def gather_kernel(
    block_ref, trailing_ref,
    t_ref, acc_ref, a_last, b_last, sum_ref,
    at, b32, a_cat, b_cat, weave, sq_mine, sq_got,
    load_sem, trailing_sem, copy_sem, y_send, y_recv, d_send, d_recv,
    tree_send, tree_recv, sq_send, sq_recv,
):
    row = lax.axis_index("row")
    col = lax.axis_index("col")
    x, z = row // 4, row % 4
    y, core = col // 2, col % 2

    def device(dx=0, dy=0, dz=0):
        return ((x + dx) % 4 * 4 + (z + dz) % 4, (y + dy) % 4 * 2 + core)

    partner = (row, y * 2 + 1 - core)
    y_up, y_down = device(dy=1), device(dy=3)
    around = (device(dx=1), device(dz=1), device(dx=3), device(dz=3))

    trailing_copy = pltpu.make_async_copy(trailing_ref, t_ref, trailing_sem)
    own = pl.multiple_of(col * 64, 64)
    load = pltpu.make_async_copy(block_ref, at.at[pl.ds(own, 64)], load_sem)
    load.start()
    barrier = pltpu.get_barrier_semaphore()
    for peer in (partner, y_up, y_down, *around):
        pl.semaphore_signal(barrier, inc=1, device_id=peer, device_id_type=MESH)
    load.wait()
    pl.semaphore_wait(barrier, 7)

    def half(y_off, same, h):
        owner = (y + y_off) % 4 * 2 + (core if same else 1 - core)
        return pl.ds(pl.multiple_of(owner * 64 + 32 * h, 32), 32)

    def send(rows, send_sem, recv_sem, to):
        return pltpu.make_async_remote_copy(
            src_ref=at.at[rows], dst_ref=at.at[rows], send_sem=send_sem, recv_sem=recv_sem,
            device_id=to, device_id_type=MESH,
        )

    for h in (0, 1):
        send(half(0, True, h), y_send.at[0], y_recv.at[2 + h], y_up).start()
        send(half(0, True, h), y_send.at[1], y_recv.at[h], y_down).start()
        send(half(0, True, h), d_send, d_recv.at[h], partner).start()

    trailing_copy.start()
    value = at[pl.ds(own, 64), :]
    square = jnp.sum((value * value).reshape(8, 8, 1280), axis=0)
    total = square[:, 0:128]
    for tile in range(1, 10):
        total = total + square[:, 128 * tile : 128 * tile + 128]
    sq_mine[0] = total

    def got_y(index, y_off, h):
        send(half(y_off, True, h), y_send.at[0], y_recv.at[index], y_up).wait_recv()

    def got_d(index, y_off, h):
        send(half(y_off, False, h), d_send, d_recv.at[index], partner).wait_recv()

    def over(index, y_off, h):
        send(half(y_off, True, h), d_send, d_recv.at[index], partner).start()

    def quarter(rel):
        return pl.ds(pl.multiple_of((y + rel) % 4 * 128, 128), 128)

    roots = []
    plans = []
    for p in range(2):
        u = (x - (y // 2 + 2 * p)) % 4
        v = (z - (y % 2 * 2 + core)) % 4
        roots.append((u == 0) & (v == 0))
        for t in range(4):
            cu, cv = ((u, v), (v, (4 - u) % 4), ((4 - u) % 4, (4 - v) % 4), ((4 - v) % 4, u))[t]
            code = look_up(cu * 4 + cv, [encode(i // 4, i % 4) for i in range(16)])
            plans.append((p, t, code % 64, code // 64 % 16, code // 1024))

    def own_copy(p, rel):
        rows = quarter(rel)
        return pltpu.make_async_copy(at.at[rows], b32.at[p, rows], copy_sem.at[p, rel])

    def convert(rel, first=0, last=10):
        if first == 0:
            for p in range(2):
                @pl.when(roots[p])
                def _():
                    own_copy(p, rel).wait()
        rows = quarter(rel)
        a_to, b_to, base = (a_last, b_last, 0) if rel == 2 else (a_cat, b_cat, 384 * (0, 1, None, 2)[rel])

        def split(value):
            high = value.astype(jnp.bfloat16)
            return high, (value - high.astype(jnp.float32)).astype(jnp.bfloat16)

        @pl.loop(first, last, unroll=5 if last - first == 10 else 2)
        def _(n):
            lanes = pl.ds(pl.multiple_of(n * 128, 128), 128)
            high, low = split(at[rows, lanes].T)
            for k, part in enumerate((high, high, low)):
                a_to[lanes, base + 128 * k : base + 128 * k + 128] = part
            for p in range(2):
                weave[n % 5, pl.ds(p, 128, stride=2), :] = b32[p, rows, lanes].T
            wide = pl.ds(pl.multiple_of(n * 256, 256), 256)
            high, low = split(weave[n % 5])
            for k, part in enumerate((high, low, high)):
                b_to[wide, base + 128 * k : base + 128 * k + 128] = part

    def product(b, start, stop):
        rows, cols = slice(256 * b, 1280), slice(512 * b, 512 * b + 512)
        return lax.dot_general(
            a_cat[rows, start:stop], b_cat[cols, start:stop],
            (((1,), (1,)), ((), ())), preferred_element_type=jnp.float32,
        )

    def multiply(start, stop, *blocks):
        for k in blocks:
            where = (slice(256 * k, 1280), slice(512 * k, 512 * k + 512))
            if start == 0:
                acc_ref[where] = product(k, start, stop)
            else:
                acc_ref[where] += product(k, start, stop)

    def ended(group):
        rows = pl.ds(0, (32, 64, 32)[group])
        for p, t, depth, kids, ends in plans:
            @pl.when(kids == 0)
            def _():
                pltpu.make_async_copy(b32.at[p, rows], b32.at[p, rows], tree_recv.at[p, t, 16 + group]).wait()

    def sq_peer(e):
        flip_x = jnp.where(e == 3, x + 1 - 2 * (x % 2), jnp.where(e == 4, 3 - x, x))
        flip_z = jnp.where(e == 5, z + 1 - 2 * (z % 2), jnp.where(e == 6, 3 - z, z))
        flip_y = jnp.where(e == 1, y + 1 - 2 * (y % 2), jnp.where(e == 2, 3 - y, y))
        flip_core = jnp.where(e == 0, 1 - core, core)
        return (flip_x * 4 + flip_z, flip_y * 2 + flip_core)

    def sq_copy(e):
        return pltpu.make_async_remote_copy(
            src_ref=sq_mine.at[e], dst_ref=sq_got.at[e], send_sem=sq_send.at[e], recv_sem=sq_recv.at[e],
            device_id=sq_peer(e), device_id_type=MESH,
        )

    def chunk_rows(c, t):
        group, low = c // 4, c % 2
        middle = (group == 1) | (group == 2)
        h = jnp.where(middle, group - 1, low)
        y_off = jnp.where(middle, 1 + 2 * low, jnp.where(group == 0, 0, 2))
        owner = (y + y_off) % 4 * 2 + (core + c // 2) % 2
        return pl.ds(pl.multiple_of(owner * 64 + 32 * h + 8 * t, 8), 8)

    @pl.loop(0, STEPS)
    def _(s):
        @pl.when(s == 2)
        def _():
            got_d(0, 0, 0)
            got_d(1, 0, 1)

        @pl.when(s == 4)
        def _():
            got_y(2, 3, 0)
            send(half(3, True, 0), y_send.at[2], y_recv.at[4], y_up).start()
            over(4, 3, 0)
            got_y(0, 1, 0)
            over(2, 1, 0)
            for p in range(2):
                @pl.when(roots[p])
                def _():
                    own_copy(p, 0).start()

        @pl.when(s == 6)
        def _():
            got_d(2, 1, 0)
            got_d(4, 3, 0)

        @pl.when(s == 8)
        def _():
            got_y(1, 1, 1)
            send(half(1, True, 1), y_send.at[3], y_recv.at[5], y_down).start()
            over(3, 1, 1)
            got_y(3, 3, 1)
            over(5, 3, 1)

        @pl.when(s == 10)
        def _():
            got_d(3, 1, 1)
            got_d(5, 3, 1)
            for p in range(2):
                @pl.when(roots[p])
                def _():
                    own_copy(p, 1).start()
                    own_copy(p, 3).start()

        @pl.when(s == 12)
        def _():
            got_y(4, 2, 0)
            over(6, 2, 0)
            got_y(5, 2, 1)
            over(7, 2, 1)

        @pl.when(s == 14)
        def _():
            got_d(6, 2, 0)
            got_d(7, 2, 1)
            for p in range(2):
                @pl.when(roots[p])
                def _():
                    own_copy(p, 2).start()

        for p, t, depth, kids, ends in plans:
            c = s - LAG * depth

            @pl.when((c >= 0) & (c < CHUNKS))
            def _():
                rows = chunk_rows(c, t)
                late = 16 + jnp.where(c >= 4, 1, 0) + jnp.where(c >= 12, 1, 0) - c

                def forward(src, d):
                    slot = c + late * (ends // (1 << d) % 2)
                    return pltpu.make_async_remote_copy(
                        src_ref=src, dst_ref=b32.at[p, rows],
                        send_sem=tree_send.at[p, t, d], recv_sem=tree_recv.at[p, t, slot],
                        device_id=around[(d + t) % 4], device_id_type=MESH,
                    )

                @pl.when(depth == 0)
                def _():
                    forward(at.at[rows], 0).start()

                @pl.when(depth > 0)
                def _():
                    pltpu.make_async_copy(b32.at[p, rows], b32.at[p, rows], tree_recv.at[p, t, c]).wait()
                    for d in range(4):
                        @pl.when(kids // (1 << d) % 2 == 1)
                        def _():
                            forward(b32.at[p, rows], d).start()

        @pl.when((s % 3 == 0) & (s < 21))
        def _():
            sq_copy(s // 3).start()

        @pl.when((s % 3 == 2) & (s < 21))
        def _():
            e = s // 3
            sq_copy(e).wait_recv()
            sq_mine[e + 1] = sq_mine[e] + sq_got[e]

        ready = 3 + LAG * (INNER + 1)

        @pl.when(s == ready)
        def _():
            ended(0)

        for k in range(5):
            @pl.when(s == ready + k)
            def _():
                convert(0, 2 * k, 2 * k + 2)

            @pl.when(s == ready + 5 + k // 2)
            def _():
                multiply(0, 384, k)

        @pl.when(s == ready + 8)
        def _():
            ended(1)
            convert(1)

        @pl.when(s == ready + 9)
        def _():
            convert(3)

        @pl.when(s == ready + 10)
        def _():
            multiply(384, 1152, 0, 1)

    multiply(384, 1152, 2, 3, 4)
    sum_ref[...] = sq_mine[7]

    def sent(sem, rows):
        return pltpu.make_async_remote_copy(
            src_ref=at.at[pl.ds(0, rows)], dst_ref=at.at[pl.ds(0, rows)], send_sem=sem, recv_sem=sem,
            device_id=partner, device_id_type=MESH,
        ).wait_send()

    for p, t, depth, kids, ends in plans:
        for d in range(4):
            @pl.when(kids // (1 << d) % 2 == 1)
            def _():
                sent(tree_send.at[p, t, d], CHUNKS * 8)

    sent(y_send.at[0], 64)
    sent(y_send.at[1], 64)
    sent(y_send.at[2], 32)
    sent(y_send.at[3], 32)
    sent(d_send, 256)

    @pl.loop(0, 7)
    def _(e):
        sq_copy(e).wait_send()

    trailing_copy.wait()

    ended(2)
    convert(2)


def update_kernel(t_ref, acc_ref, a_ref, b_ref, sum_ref, out_ref, stage, upper_sem, lower_sem):
    row = lax.axis_index("row")
    col = lax.axis_index("col")

    def upper(a):
        where = (pl.ds(256 * a, 256), pl.ds(512 * (a + 1), 2560 - 512 * (a + 1)))
        return pltpu.make_async_copy(t_ref.at[where], out_ref.at[where], upper_sem.at[a])

    def lower(b):
        where = (pl.ds(256 * b, 1280 - 256 * b), pl.ds(512 * b, 512))
        return pltpu.make_async_copy(stage.at[where], out_ref.at[where], lower_sem.at[b])

    for a in range(4):
        upper(a).start()
    squares = jnp.full((8, 512), jnp.sum(sum_ref[...]), jnp.float32)
    factor = (0.8 * jnp.sqrt(jnp.float32(N)) / jnp.sqrt(squares + 1e-6))[0:1, :]
    i = lax.broadcasted_iota(jnp.int32, (256, 512), 0)
    j = lax.broadcasted_iota(jnp.int32, (256, 512), 1)
    for b in range(5):
        cols = slice(512 * b, 512 * b + 512)
        update = acc_ref[256 * b : 1280, cols] + lax.dot_general(
            a_ref[256 * b : 1280, :], b_ref[cols, :],
            (((1,), (1,)), ((), ())), preferred_element_type=jnp.float32,
        )
        edge = slice(256 * b, 256 * b + 256)
        below = (256 * b + i) * 16 + row >= (512 * b + j) * 8 + col
        stage[edge, cols] = t_ref[edge, cols] - factor * jnp.where(below, update[0:256], 0.0)
        if b < 4:
            rest = slice(256 * b + 256, 1280)
            stage[rest, cols] = t_ref[rest, cols] - factor * update[256:]
        lower(b).start()
    for a in range(4):
        upper(a).wait()
    for b in range(5):
        lower(b).wait()


def on_device(panel_block, trailing):
    bf16 = jnp.bfloat16
    f32 = jnp.float32
    dma = pltpu.SemaphoreType.DMA
    anywhere = pl.BlockSpec(memory_space=pl.ANY)
    in_hbm = functools.partial(pltpu.with_memory_space_constraint, memory_space=pltpu.HBM)
    vmem = pl.BlockSpec(memory_space=pltpu.VMEM)
    gathered = pl.pallas_call(
        gather_kernel,
        out_shape=(
            pltpu.VMEM((1280, 2560), f32),
            pltpu.VMEM((1280, 2560), f32),
            pltpu.VMEM((1280, 384), bf16),
            pltpu.VMEM((2560, 384), bf16),
            pltpu.VMEM((8, 128), f32),
        ),
        in_specs=[anywhere, anywhere],
        out_specs=[vmem] * 5,
        scratch_shapes=[
            pltpu.VMEM((512, 1280), f32),
            pltpu.VMEM((2, 512, 1280), f32),
            pltpu.VMEM((1280, 1152), bf16),
            pltpu.VMEM((2560, 1152), bf16),
            pltpu.VMEM((5, 256, 128), f32),
            pltpu.VMEM((8, 8, 128), f32),
            pltpu.VMEM((7, 8, 128), f32),
            dma(()), dma(()), dma((2, 4)), dma((4,)), dma((6,)), dma(()), dma((8,)),
            dma((2, 4, 4)), dma((2, 4, CHUNKS + 3)), dma((7,)), dma((7,)),
        ],
        compiler_params=pltpu.CompilerParams(
            collective_id=0, has_side_effects=True, vmem_limit_bytes=24 * 1024 * 1024
        ),
        name="gather",
    )(in_hbm(panel_block.T), in_hbm(trailing))
    return pl.pallas_call(
        update_kernel,
        out_shape=jax.ShapeDtypeStruct((1280, 2560), f32),
        in_specs=[vmem] * 5,
        out_specs=anywhere,
        scratch_shapes=[pltpu.VMEM((1280, 2560), f32), dma((4,)), dma((5,))],
        compiler_params=pltpu.CompilerParams(vmem_limit_bytes=24 * 1024 * 1024),
        name="update",
    )(*gathered)


def solution(mesh):
    return jax.shard_map(
        on_device,
        mesh=mesh,
        in_specs=(P("row", "col"), P("row", "col")),
        out_specs=P("row", "col"),
        check_vma=False,
    )
```

```python
import functools

import jax
import jax.numpy as jnp
from jax import lax
from jax.experimental import pallas as pl
from jax.experimental.pallas import tpu as pltpu
from jax.sharding import PartitionSpec as P

N = 20480
MESH = pl.DeviceIdType.MESH
LAG = 2
CHUNKS = 16
INNER = 4
STEPS = CHUNKS + LAG * INNER
TREE = {
    (0, 0): (0, (0,)),
    (1, 0): (1, (0, 1, 3)),
    (1, 3): (2, (0, 2, 3)),
    (1, 1): (2, (2,)),
    (2, 0): (2, (0, 1)),
    (2, 3): (3, (0,)),
    (1, 2): (3, (2,)),
    (0, 1): (3, ()),
    (0, 3): (3, ()),
    (2, 1): (3, (0, 1)),
    (3, 0): (3, ()),
    (2, 2): (4, (0,)),
    (0, 2): (4, ()),
    (3, 1): (4, ()),
    (3, 3): (4, ()),
    (3, 2): (5, ()),
}


def encode(u, v):
    depth, kids = TREE[u, v]
    step = ((1, 0), (0, 1), (3, 0), (0, 3))
    ends = [k for k in kids if not TREE[(u + step[k][0]) % 4, (v + step[k][1]) % 4][1]]
    if not kids:
        depth = 63
    return depth + 64 * sum(1 << k for k in kids) + 1024 * sum(1 << k for k in ends)


def look_up(index, table):
    found = jnp.int32(0)
    for key, value in enumerate(table):
        found = jnp.where(index == key, jnp.int32(value), found)
    return found


def gather_kernel(
    block_ref, trailing_ref,
    t_ref, acc_ref, a_last, b_last, sum_ref,
    at, b32, a_cat, b_cat, weave, sq_mine, sq_got,
    load_sem, trailing_sem, copy_sem, y_send, y_recv, d_send, d_recv,
    tree_send, tree_recv, sq_send, sq_recv,
):
    row = lax.axis_index("row")
    col = lax.axis_index("col")
    x, z = row // 4, row % 4
    y, core = col // 2, col % 2

    def device(dx=0, dy=0, dz=0):
        return ((x + dx) % 4 * 4 + (z + dz) % 4, (y + dy) % 4 * 2 + core)

    partner = (row, y * 2 + 1 - core)
    y_up, y_down = device(dy=1), device(dy=3)
    around = (device(dx=1), device(dz=1), device(dx=3), device(dz=3))

    trailing_copy = pltpu.make_async_copy(trailing_ref, t_ref, trailing_sem)
    own = pl.multiple_of(col * 64, 64)
    load = pltpu.make_async_copy(block_ref, at.at[pl.ds(own, 64)], load_sem)
    load.start()
    barrier = pltpu.get_barrier_semaphore()
    for peer in (partner, y_up, y_down, *around):
        pl.semaphore_signal(barrier, inc=1, device_id=peer, device_id_type=MESH)
    load.wait()
    pl.semaphore_wait(barrier, 7)

    def half(y_off, same, h):
        owner = (y + y_off) % 4 * 2 + (core if same else 1 - core)
        return pl.ds(pl.multiple_of(owner * 64 + 32 * h, 32), 32)

    def send(rows, send_sem, recv_sem, to):
        return pltpu.make_async_remote_copy(
            src_ref=at.at[rows], dst_ref=at.at[rows], send_sem=send_sem, recv_sem=recv_sem,
            device_id=to, device_id_type=MESH,
        )

    for h in (0, 1):
        send(half(0, True, h), y_send.at[0], y_recv.at[2 + h], y_up).start()
        send(half(0, True, h), y_send.at[1], y_recv.at[h], y_down).start()
        send(half(0, True, h), d_send, d_recv.at[h], partner).start()

    trailing_copy.start()

    def got_y(index, y_off, h):
        send(half(y_off, True, h), y_send.at[0], y_recv.at[index], y_up).wait_recv()

    def got_d(index, y_off, h):
        send(half(y_off, False, h), d_send, d_recv.at[index], partner).wait_recv()

    def over(index, y_off, h):
        send(half(y_off, True, h), d_send, d_recv.at[index], partner).start()

    def quarter(rel):
        return pl.ds(pl.multiple_of((y + rel) % 4 * 128, 128), 128)

    roots = []
    plans = []
    for p in range(2):
        u = (x - (y // 2 + 2 * p)) % 4
        v = (z - (y % 2 * 2 + core)) % 4
        roots.append((u == 0) & (v == 0))
        for t in range(4):
            cu, cv = ((u, v), (v, (4 - u) % 4), ((4 - u) % 4, (4 - v) % 4), ((4 - v) % 4, u))[t]
            code = look_up(cu * 4 + cv, [encode(i // 4, i % 4) for i in range(16)])
            plans.append((p, t, code % 64, code // 64 % 16, code // 1024))

    def own_copy(p, rel):
        rows = quarter(rel)
        return pltpu.make_async_copy(at.at[rows], b32.at[p, rows], copy_sem.at[p, rel])

    def convert(rel, first=0, last=10):
        if first == 0:
            for p in range(2):
                @pl.when(roots[p])
                def _():
                    own_copy(p, rel).wait()
        rows = quarter(rel)
        a_to, b_to, base = (a_last, b_last, 0) if rel == 2 else (a_cat, b_cat, 384 * (0, 1, None, 2)[rel])

        def split(value):
            high = value.astype(jnp.bfloat16)
            return high, (value - high.astype(jnp.float32)).astype(jnp.bfloat16)

        @pl.loop(first, last, unroll=5 if last - first == 10 else 2)
        def _(n):
            lanes = pl.ds(pl.multiple_of(n * 128, 128), 128)
            high, low = split(at[rows, lanes].T)
            for k, part in enumerate((high, high, low)):
                a_to[lanes, base + 128 * k : base + 128 * k + 128] = part
            for p in range(2):
                weave[n % 5, pl.ds(p, 128, stride=2), :] = b32[p, rows, lanes].T
            wide = pl.ds(pl.multiple_of(n * 256, 256), 256)
            high, low = split(weave[n % 5])
            for k, part in enumerate((high, low, high)):
                b_to[wide, base + 128 * k : base + 128 * k + 128] = part

    def product(b, start, stop):
        rows, cols = slice(256 * b, 1280), slice(512 * b, 512 * b + 512)
        return lax.dot_general(
            a_cat[rows, start:stop], b_cat[cols, start:stop],
            (((1,), (1,)), ((), ())), preferred_element_type=jnp.float32,
        )

    def multiply(start, stop, *blocks):
        for k in blocks:
            where = (slice(256 * k, 1280), slice(512 * k, 512 * k + 512))
            if start == 0:
                acc_ref[where] = product(k, start, stop)
            else:
                acc_ref[where] += product(k, start, stop)

    def ended(group):
        rows = pl.ds(0, (32, 64, 32)[group])
        for p, t, depth, kids, ends in plans:
            @pl.when(kids == 0)
            def _():
                pltpu.make_async_copy(b32.at[p, rows], b32.at[p, rows], tree_recv.at[p, t, 16 + group]).wait()

    def sq_peer(e):
        flip_x = jnp.where(e == 3, x + 1 - 2 * (x % 2), jnp.where(e == 4, 3 - x, x))
        flip_z = jnp.where(e == 5, z + 1 - 2 * (z % 2), jnp.where(e == 6, 3 - z, z))
        flip_y = jnp.where(e == 1, y + 1 - 2 * (y % 2), jnp.where(e == 2, 3 - y, y))
        flip_core = jnp.where(e == 0, 1 - core, core)
        return (flip_x * 4 + flip_z, flip_y * 2 + flip_core)

    def sq_copy(e):
        return pltpu.make_async_remote_copy(
            src_ref=sq_mine.at[e], dst_ref=sq_got.at[e], send_sem=sq_send.at[e], recv_sem=sq_recv.at[e],
            device_id=sq_peer(e), device_id_type=MESH,
        )

    def chunk_rows(c, t):
        group, low = c // 4, c % 2
        middle = (group == 1) | (group == 2)
        h = jnp.where(middle, group - 1, low)
        y_off = jnp.where(middle, 1 + 2 * low, jnp.where(group == 0, 0, 2))
        owner = (y + y_off) % 4 * 2 + (core + c // 2) % 2
        return pl.ds(pl.multiple_of(owner * 64 + 32 * h + 8 * t, 8), 8)

    @pl.loop(0, STEPS)
    def _(s):
        @pl.when(s == 2)
        def _():
            got_d(0, 0, 0)
            got_d(1, 0, 1)

        @pl.when(s == 4)
        def _():
            got_y(2, 3, 0)
            send(half(3, True, 0), y_send.at[2], y_recv.at[4], y_up).start()
            over(4, 3, 0)
            got_y(0, 1, 0)
            over(2, 1, 0)
            for p in range(2):
                @pl.when(roots[p])
                def _():
                    own_copy(p, 0).start()

        @pl.when(s == 6)
        def _():
            got_d(2, 1, 0)
            got_d(4, 3, 0)

        @pl.when(s == 8)
        def _():
            got_y(1, 1, 1)
            send(half(1, True, 1), y_send.at[3], y_recv.at[5], y_down).start()
            over(3, 1, 1)
            got_y(3, 3, 1)
            over(5, 3, 1)

        @pl.when(s == 10)
        def _():
            got_d(3, 1, 1)
            got_d(5, 3, 1)
            for p in range(2):
                @pl.when(roots[p])
                def _():
                    own_copy(p, 1).start()
                    own_copy(p, 3).start()

        @pl.when(s == 12)
        def _():
            got_y(4, 2, 0)
            over(6, 2, 0)
            got_y(5, 2, 1)
            over(7, 2, 1)

        @pl.when(s == 14)
        def _():
            got_d(6, 2, 0)
            got_d(7, 2, 1)
            for p in range(2):
                @pl.when(roots[p])
                def _():
                    own_copy(p, 2).start()

        for p, t, depth, kids, ends in plans:
            c = s - LAG * depth

            @pl.when((c >= 0) & (c < CHUNKS))
            def _():
                rows = chunk_rows(c, t)
                late = 16 + jnp.where(c >= 4, 1, 0) + jnp.where(c >= 12, 1, 0) - c

                def forward(src, d):
                    slot = c + late * (ends // (1 << d) % 2)
                    return pltpu.make_async_remote_copy(
                        src_ref=src, dst_ref=b32.at[p, rows],
                        send_sem=tree_send.at[p, t, d], recv_sem=tree_recv.at[p, t, slot],
                        device_id=around[(d + t) % 4], device_id_type=MESH,
                    )

                @pl.when(depth == 0)
                def _():
                    forward(at.at[rows], 0).start()

                @pl.when(depth > 0)
                def _():
                    pltpu.make_async_copy(b32.at[p, rows], b32.at[p, rows], tree_recv.at[p, t, c]).wait()
                    for d in range(4):
                        @pl.when(kids // (1 << d) % 2 == 1)
                        def _():
                            forward(b32.at[p, rows], d).start()

        @pl.when(s == 0)
        def _():
            value = at[pl.ds(own, 64), :]
            square = jnp.sum((value * value).reshape(8, 8, 1280), axis=0)
            total = square[:, 0:128]
            for tile in range(1, 10):
                total = total + square[:, 128 * tile : 128 * tile + 128]
            sq_mine[0] = total

        @pl.when((s % 3 == 1) & (s < 20))
        def _():
            sq_copy(s // 3).start()

        @pl.when((s % 3 == 0) & (s > 0) & (s < 22))
        def _():
            e = s // 3 - 1
            sq_copy(e).wait_recv()
            sq_mine[e + 1] = sq_mine[e] + sq_got[e]

        ready = 3 + LAG * (INNER + 1)

        @pl.when(s == ready)
        def _():
            ended(0)

        for k in range(5):
            @pl.when(s == ready + k)
            def _():
                convert(0, 2 * k, 2 * k + 2)

            @pl.when(s == ready + 5 + k // 2)
            def _():
                multiply(0, 384, k)

        @pl.when(s == ready + 8)
        def _():
            ended(1)
            convert(1)

        @pl.when(s == ready + 9)
        def _():
            convert(3)

        @pl.when(s == ready + 10)
        def _():
            multiply(384, 1152, 0, 1)

    multiply(384, 1152, 2, 3, 4)
    sum_ref[...] = sq_mine[7]

    def sent(sem, rows):
        return pltpu.make_async_remote_copy(
            src_ref=at.at[pl.ds(0, rows)], dst_ref=at.at[pl.ds(0, rows)], send_sem=sem, recv_sem=sem,
            device_id=partner, device_id_type=MESH,
        ).wait_send()

    for p, t, depth, kids, ends in plans:
        for d in range(4):
            @pl.when(kids // (1 << d) % 2 == 1)
            def _():
                sent(tree_send.at[p, t, d], CHUNKS * 8)

    sent(y_send.at[0], 64)
    sent(y_send.at[1], 64)
    sent(y_send.at[2], 32)
    sent(y_send.at[3], 32)
    sent(d_send, 256)

    @pl.loop(0, 7)
    def _(e):
        sq_copy(e).wait_send()

    trailing_copy.wait()

    ended(2)
    convert(2)


def update_kernel(t_ref, acc_ref, a_ref, b_ref, sum_ref, out_ref, stage, upper_sem, lower_sem):
    row = lax.axis_index("row")
    col = lax.axis_index("col")

    def upper(a):
        where = (pl.ds(256 * a, 256), pl.ds(512 * (a + 1), 2560 - 512 * (a + 1)))
        return pltpu.make_async_copy(t_ref.at[where], out_ref.at[where], upper_sem.at[a])

    def lower(b):
        where = (pl.ds(256 * b, 1280 - 256 * b), pl.ds(512 * b, 512))
        return pltpu.make_async_copy(stage.at[where], out_ref.at[where], lower_sem.at[b])

    for a in range(4):
        upper(a).start()
    squares = jnp.full((8, 512), jnp.sum(sum_ref[...]), jnp.float32)
    factor = (0.8 * jnp.sqrt(jnp.float32(N)) / jnp.sqrt(squares + 1e-6))[0:1, :]
    i = lax.broadcasted_iota(jnp.int32, (256, 512), 0)
    j = lax.broadcasted_iota(jnp.int32, (256, 512), 1)
    for b in range(5):
        cols = slice(512 * b, 512 * b + 512)
        update = acc_ref[256 * b : 1280, cols] + lax.dot_general(
            a_ref[256 * b : 1280, :], b_ref[cols, :],
            (((1,), (1,)), ((), ())), preferred_element_type=jnp.float32,
        )
        edge = slice(256 * b, 256 * b + 256)
        below = (256 * b + i) * 16 + row >= (512 * b + j) * 8 + col
        stage[edge, cols] = t_ref[edge, cols] - factor * jnp.where(below, update[0:256], 0.0)
        if b < 4:
            rest = slice(256 * b + 256, 1280)
            stage[rest, cols] = t_ref[rest, cols] - factor * update[256:]
        lower(b).start()
    for a in range(4):
        upper(a).wait()
    for b in range(5):
        lower(b).wait()


def on_device(panel_block, trailing):
    bf16 = jnp.bfloat16
    f32 = jnp.float32
    dma = pltpu.SemaphoreType.DMA
    anywhere = pl.BlockSpec(memory_space=pl.ANY)
    in_hbm = functools.partial(pltpu.with_memory_space_constraint, memory_space=pltpu.HBM)
    vmem = pl.BlockSpec(memory_space=pltpu.VMEM)
    gathered = pl.pallas_call(
        gather_kernel,
        out_shape=(
            pltpu.VMEM((1280, 2560), f32),
            pltpu.VMEM((1280, 2560), f32),
            pltpu.VMEM((1280, 384), bf16),
            pltpu.VMEM((2560, 384), bf16),
            pltpu.VMEM((8, 128), f32),
        ),
        in_specs=[anywhere, anywhere],
        out_specs=[vmem] * 5,
        scratch_shapes=[
            pltpu.VMEM((512, 1280), f32),
            pltpu.VMEM((2, 512, 1280), f32),
            pltpu.VMEM((1280, 1152), bf16),
            pltpu.VMEM((2560, 1152), bf16),
            pltpu.VMEM((5, 256, 128), f32),
            pltpu.VMEM((8, 8, 128), f32),
            pltpu.VMEM((7, 8, 128), f32),
            dma(()), dma(()), dma((2, 4)), dma((4,)), dma((6,)), dma(()), dma((8,)),
            dma((2, 4, 4)), dma((2, 4, CHUNKS + 3)), dma((7,)), dma((7,)),
        ],
        compiler_params=pltpu.CompilerParams(
            collective_id=0, has_side_effects=True, vmem_limit_bytes=24 * 1024 * 1024
        ),
        name="gather",
    )(in_hbm(panel_block.T), in_hbm(trailing))
    return pl.pallas_call(
        update_kernel,
        out_shape=jax.ShapeDtypeStruct((1280, 2560), f32),
        in_specs=[vmem] * 5,
        out_specs=anywhere,
        scratch_shapes=[pltpu.VMEM((1280, 2560), f32), dma((4,)), dma((5,))],
        compiler_params=pltpu.CompilerParams(vmem_limit_bytes=24 * 1024 * 1024),
        name="update",
    )(*gathered)


def solution(mesh):
    return jax.shard_map(
        on_device,
        mesh=mesh,
        in_specs=(P("row", "col"), P("row", "col")),
        out_specs=P("row", "col"),
        check_vma=False,
    )
```
